512 devices in a mesh: rows: 128 (over z, y_lo, x), cols: 4 (over y_hi, core).
Axes of the slice: x: 4, y: 4 (y_hi: 2, y_lo: 2; y = y_hi * 2 + y_lo), z: 16, core: 2. Of those that a mesh axis runs over, the one named last changes fastest.
Arguments:
- lattice: int32 [4096, 16384], P('rows', 'cols'), may hold values from -1 to 1, as said below
- draws: int32 [2, 4096, 16384], P(None, 'rows', 'cols'), may hold values from -2147483648 to 2147483647, as said below
- thresholds: int32 [5], replicated, may hold values from 32 to 256
Outputs:
- final_lattice: int32 [4096, 16384], P('rows', 'cols')
- row_magnetization: float32 [4096], P('rows')
The draws below stay inside these ranges and needn't reach their ends.
Inputs may be any that keep to these rules, and one draw needn't show every extreme that they name: `lattice`: every entry is -1 or 1. Each word holds four independent draws of 0 to 255: bits 8k to 8k+7 of draws[p] belong to sweep 4p + k.
All inputs are finite; a program needn't handle non-finite values.
Results may differ from the reference program's by a relative error of at most 0.0003.
Values sent between devices are 32-bit elements; how exact they have to be, the bound alone decides.
No kernel may reach another device: no remote copies, remote signals or barrier semaphores. Data moves between devices by JAX's collectives and lax.ppermute only.
A program may use at most 64 MiB of HBM per device.

```python
import jax
import jax.numpy as jnp
from jax import lax

SWEEPS = 8
LEVELS = 5
NX = 4096
NY = 16384
PACKS = 2


def draw_lattice(key, part):
    picks = jax.random.randint(jax.random.fold_in(key, 11), (NX, NY), 0, 20 * NX, dtype=jnp.int32)
    row_ids = lax.broadcasted_iota(jnp.int32, (NX, NY), 0)
    return jnp.where(picks < 11 * NX + 8 * row_ids, 1, -1).astype(jnp.int32)


def draw_draws(key, part):
    return jax.random.randint(jax.random.fold_in(key, 23), (PACKS, NX, NY), -2147483648, 2147483647, dtype=jnp.int32)


def plant(entries, own_key, least, top_value):
    shape = entries.shape
    spot = [jax.random.randint(jax.random.fold_in(own_key, axis), (), 0, shape[axis]) for axis in range(len(shape))]
    entries = entries.at[tuple(spot)].set(least)
    longest = shape.index(max(shape))
    spot[longest] = (spot[longest] + 1) % shape[longest]
    return entries.at[tuple(spot)].set(top_value)


def setup_inputs(seed: int = 0) -> dict:
    splits = jax.random.split(jax.random.key(seed), 4)
    lattice = draw_lattice(jax.random.fold_in(splits[3], 71), 0)
    draws = draw_draws(jax.random.fold_in(splits[3], 71), 0)
    thresholds = plant(jax.random.randint(splits[2], (LEVELS,), 32, 257), jax.random.fold_in(splits[2], 1), 32, 256).astype(jnp.int32)
    return dict(lattice=lattice, draws=draws, thresholds=thresholds)


def reference(lattice, draws, thresholds):
    spins_now = lattice
    row_ids = lax.broadcasted_iota(jnp.int32, lattice.shape, 0)
    col_ids = lax.broadcasted_iota(jnp.int32, lattice.shape, 1)
    parity = (row_ids + col_ids) % 2
    for sweep_no in range(SWEEPS):
        draw_bytes = (draws[sweep_no // 4] >> (8 * (sweep_no % 4))) & 255
        for colour in (0, 1):
            neighbours = (jnp.roll(spins_now, 1, 0) + jnp.roll(spins_now, -1, 0)
                          + jnp.roll(spins_now, 1, 1) + jnp.roll(spins_now, -1, 1))
            level = (spins_now * neighbours + 4) // 2
            allowed = jnp.zeros_like(spins_now)
            for entry in range(LEVELS):
                allowed = jnp.where(level == entry, thresholds[entry], allowed)
            flipped = (parity == colour) & (draw_bytes < allowed)
            spins_now = jnp.where(flipped, -spins_now, spins_now)
    means = jnp.sum(spins_now.astype(jnp.float32), axis=1) / NY
    return spins_now, means
```

```python
import jax
import jax.numpy as jnp
from jax import lax
from jax.experimental import pallas as pl
from jax.experimental.pallas import tpu as pltpu
from jax.sharding import PartitionSpec as P

SWEEPS = 8
LEVELS = 5
GROUPS = 32
LANES = 128
I32 = jnp.int32


def iotas():
    sub = lax.broadcasted_iota(I32, (8, LANES), 0)
    lane = lax.broadcasted_iota(I32, (8, LANES), 1)
    return sub, lane, (sub + lane) % 2 == 0


def srl(x, n):
    return lax.shift_right_logical(x, jnp.full(x.shape, n, I32))


def up_one(x):
    return pltpu.roll(x, 7, 0)


def split_colours(first, second, even):
    moved = up_one(second)
    return jnp.where(even, first, moved), jnp.where(even, moved, first)


def transpose_bits(words, low_half=False):
    a = list(words)
    masks = {16: 0x0000FFFF, 8: 0x00FF00FF, 4: 0x0F0F0F0F, 2: 0x33333333, 1: 0x55555555}
    for j in (16, 8, 4, 2, 1):
        m = jnp.int32(masks[j])
        for k in range(32):
            if k & j:
                continue
            if low_half and j == 16:
                a[k], a[k + j] = a[k] & m, srl(a[k], 16)
                continue
            t = (srl(a[k], j) ^ a[k + j]) & m
            a[k + j] = a[k + j] ^ t
            a[k] = a[k] ^ (t << j)
    return a


def pack_spins(load):
    word = srl(load(0), 1) & 1
    for g in range(1, GROUPS):
        bit = 1 << g if g < 31 else -(1 << 31)
        word = word | (load(g) & jnp.int32(bit))
    return word


def own_kernel(lattice, draws, planes, words):
    _, _, even = iotas()

    def tile(ref, row, g):
        return ref[pl.ds(row, 8), pl.ds(g * LANES, LANES)]

    for q in range(2):
        first = pack_spins(lambda g: tile(lattice, 16 * q, g))
        second = pack_spins(lambda g: tile(lattice, 16 * q + 8, g))
        words[q, 0], words[q, 1] = split_colours(first, second, even)

    def body(n, carry):
        q, p = n // 2, n % 2
        row = pl.multiple_of(q * 16, 16)
        pairs = []
        for g in range(GROUPS):
            cols = pl.ds(g * LANES, LANES)
            pairs.append(split_colours(draws[p, pl.ds(row, 8), cols], draws[p, pl.ds(row + 8, 8), cols], even))
        for c in range(2):
            for b, plane in enumerate(transpose_bits([pair[c] for pair in pairs])):
                planes[q, c, p, b] = plane
        return carry

    lax.fori_loop(0, 4, body, 0)


def sweep_kernel(thresholds, top, bot, h_top, h_own, h_bot, words, planes, final, means, edge0, edge1, side):
    sub, lane, even = iotas()
    odd = jnp.logical_not(even)

    def tile(ref, row, g):
        return ref[pl.ds(row, 8), pl.ds(g * LANES, LANES)]

    state = [[None] * 5, [None] * 5]
    for q, ref in ((0, top), (3, bot)):
        first = pack_spins(lambda g: tile(ref, 0, g))
        second = pack_spins(lambda g: tile(ref, 8, g))
        state[0][q], state[1][q] = split_colours(first, second, even)
    for q in (1, 2):
        for c in range(2):
            state[c][q] = words[q - 1, c]
    side_rows = ((h_top, 0), (h_own, 0), (h_own, 16), (h_bot, 0))
    state[0][4] = state[1][4] = jnp.zeros((8, LANES), I32)
    for q, (ref, row) in enumerate(side_rows):
        pair = split_colours(ref[pl.ds(row, 8), :], ref[pl.ds(row + 8, 8), :], even)
        for c in range(2):
            state[c][4] = state[c][4] | ((srl(pair[c], 1) & 1) << q)

    for n, ref in enumerate((top, bot)):
        pairs = [split_colours(tile(ref, 16, g), tile(ref, 24, g), even) for g in range(GROUPS)]
        for c in range(2):
            for b, plane in enumerate(transpose_bits([pair[c] for pair in pairs])):
                edge0[n, c, b] = plane
    pairs = [split_colours(tile(bot, 32, g), tile(top, 32, g), even) for g in range(GROUPS)]
    for c in range(2):
        for b, plane in enumerate(transpose_bits([pair[c] for pair in pairs])):
            edge1[c, b] = plane
    slots = [jnp.zeros((8, LANES), I32)] * 32
    first_word = ((h_top, 16), (h_own, 32), (h_own, 48), (h_bot, 16))
    for q, (ref, row) in enumerate(first_word):
        slots[q], slots[4 + q] = split_colours(ref[pl.ds(row, 8), :], ref[pl.ds(row + 8, 8), :], even)
    joined = split_colours(h_bot[pl.ds(32, 8), :], h_top[pl.ds(32, 8), :], even)
    for q in range(4):
        if q in (0, 3):
            slots[8 + q], slots[12 + q] = joined
        else:
            row = 64 + 16 * (q - 1)
            slots[8 + q], slots[12 + q] = split_colours(
                h_own[pl.ds(row, 8), :], h_own[pl.ds(row + 8, 8), :], even
            )
    for b, plane in enumerate(transpose_bits(slots, low_half=True)):
        side[b] = plane

    table = []
    for b in range(8):
        r = [-(((thresholds[4 - k] - 1) >> b) & 1) for k in range(LEVELS)]
        table.append((r[0], r[0] ^ r[1], r[0] ^ r[2], r[0] ^ r[1] ^ r[2] ^ r[3], r[0] ^ r[4]))

    at_left, at_right = lane == 0, lane == LANES - 1
    fix = []
    for c in range(2):
        here, there = (even, odd) if c == 0 else (odd, even)
        fix.append(
            (here & (sub == 0), there & (sub == 7), here & (sub == 7), there & (sub == 6))
        )

    def half_sweep(mine, other, c, draw):
        up_prev, up_self, down_self, down_next = fix[c]
        left = [pltpu.roll(w, 1, 1) for w in other]
        right = [pltpu.roll(w, LANES - 1, 1) for w in other]
        side_left = srl(left[0], 31)
        side_right = right[0] & 1
        for q in range(1, 4):
            side_left = side_left | (srl(left[q], 31) << q)
            side_right = side_right | ((right[q] & 1) << q)
        new = []
        for q in range(5):
            w = other[q]
            if q < 4:
                from_side = srl(left[4], q) & 1
                lft = jnp.where(at_left, (left[q] << 1) | from_side, left[q])
                from_side = (right[4] << (31 - q)) & jnp.int32(-(1 << 31))
                rgt = jnp.where(at_right, srl(right[q], 1) | from_side, right[q])
                before = pltpu.roll(other[max(q - 1, 0)], 2, 0)
                after = pltpu.roll(other[min(q + 1, 3)], 6, 0)
            else:
                lft = jnp.where(at_left, side_left, left[4])
                rgt = jnp.where(at_right, side_right, right[4])
                before = pltpu.roll(w, 2, 0) << 1
                after = srl(pltpu.roll(w, 6, 0), 1)
            up = jnp.where(up_prev, before, jnp.where(up_self, w, pltpu.roll(w, 1, 0)))
            down = jnp.where(down_next, after, jnp.where(down_self, w, pltpu.roll(w, 7, 0)))
            s = mine[q]
            lft, rgt, up, down = lft ^ s, rgt ^ s, up ^ s, down ^ s
            s1, c1 = lft ^ rgt, lft & rgt
            s2, c2 = up ^ down, up & down
            k0 = s1 ^ s2
            k1 = (c1 ^ c2) | (s1 & s2)
            k2 = c1 & c2
            k01 = k0 & k1
            above = None
            for b in range(8):
                x = table[b]
                limit = x[0] ^ (k0 & x[1]) ^ (k1 & x[2]) ^ (k01 & x[3]) ^ (k2 & x[4])
                u = draw(q, b)
                above = u & ~limit if above is None else above ^ ((u ^ limit) & (above ^ u))
            new.append(~(s ^ above))
        return new

    def sweep(p, t, a, b):
        def draw(c):
            def plane(q, bit):
                at = 8 * t + bit
                if q == 4:
                    return srl(side[at], 8 * p + 4 * c)
                if q in (1, 2):
                    return planes[q - 1, c, p, at]
                return edge0[q // 3, c, at] if p == 0 else edge1[c, at]

            return plane

        a = half_sweep(a, b, 0, draw(0))
        b = half_sweep(b, a, 1, draw(1))
        return a, b

    a, b = state
    for p in range(2):
        a, b = lax.fori_loop(0, 4, lambda t, ab: sweep(p, t, *ab), (a, b))

    sums = jnp.zeros((8, LANES), jnp.float32)
    for q in (1, 2):
        first = jnp.where(even, a[q], b[q])
        moved = jnp.where(even, b[q], a[q])
        second = pltpu.roll(moved, 1, 0)
        for n, word in enumerate((first, second)):
            row = 16 * (q - 1) + 8 * n
            minus = jnp.sum(lax.population_count(word).astype(jnp.float32), axis=1, keepdims=True)
            mean = (GROUPS * LANES - 2.0 * minus) * (1.0 / (4 * GROUPS * LANES))
            sums = sums + jnp.where(lane == row + sub, mean, 0.0)
            for g in range(GROUPS):
                spin = ((word << (31 - g)) >> 31) | 1
                final[pl.ds(row, 8), pl.ds(g * LANES, LANES)] = spin
    means[...] = jnp.sum(sums, axis=0, keepdims=True)[:, :32]


def shift(x, axis, by):
    count = lax.axis_size(axis)
    return lax.ppermute(x, axis, [(i, (i + by) % count) for i in range(count)])


def on_device(lattice, draws, thresholds):
    down = jnp.concatenate([lattice[16:], draws[0, 16:], draws[1, 24:]], axis=0)
    up = jnp.concatenate([lattice[:16], draws[0, :16], draws[1, :8]], axis=0)
    top = shift(down, "rows", 1)
    bot = shift(up, "rows", -1)
    stacked = jnp.concatenate([lattice, draws[0], draws[1]], axis=0)
    from_left = shift(stacked[:, -LANES:], "cols", 1)
    from_right = shift(stacked[:, :LANES], "cols", -1)
    lane = lax.broadcasted_iota(I32, (1, LANES), 1)
    side = jnp.where(lane < LANES // 2, from_right, from_left)
    h_top = shift(jnp.concatenate([side[16:32], side[48:64], side[88:]], axis=0), "rows", 1)
    h_bot = shift(jnp.concatenate([side[:16], side[32:48], side[64:72]], axis=0), "rows", -1)

    planes, words = pl.pallas_call(
        own_kernel,
        out_shape=(
            jax.ShapeDtypeStruct((2, 2, 2, 32, 8, LANES), I32),
            jax.ShapeDtypeStruct((2, 2, 8, LANES), I32),
        ),
        cost_estimate=pl.CostEstimate(flops=30_000_000, bytes_accessed=2_700_000, transcendentals=0),
    )(lattice, draws)
    vmem = pl.BlockSpec(memory_space=pltpu.VMEM)
    final, means = pl.pallas_call(
        sweep_kernel,
        out_shape=(
            jax.ShapeDtypeStruct((32, GROUPS * LANES), I32),
            jax.ShapeDtypeStruct((1, 32), jnp.float32),
        ),
        in_specs=[pl.BlockSpec(memory_space=pltpu.SMEM)] + [vmem] * 7,
        scratch_shapes=[
            pltpu.VMEM((2, 2, 32, 8, LANES), I32),
            pltpu.VMEM((2, 32, 8, LANES), I32),
            pltpu.VMEM((32, 8, LANES), I32),
        ],
        cost_estimate=pl.CostEstimate(flops=40_000_000, bytes_accessed=2_700_000, transcendentals=0),
    )(thresholds, top, bot, h_top, side, h_bot, words, planes)
    return final, lax.psum(means, "cols").reshape(32)


def solution(mesh):
    in_specs = (P("rows", "cols"), P(None, "rows", "cols"), P())
    out_specs = (P("rows", "cols"), P("rows"))
    return jax.shard_map(
        on_device, mesh=mesh, in_specs=in_specs, out_specs=out_specs, check_vma=False
    )
```

```python
import jax
import jax.numpy as jnp
from jax import lax
from jax.experimental import pallas as pl
from jax.experimental.pallas import tpu as pltpu
from jax.sharding import PartitionSpec as P

SWEEPS = 8
LEVELS = 5
GROUPS = 32
LANES = 128
I32 = jnp.int32


def iotas():
    sub = lax.broadcasted_iota(I32, (8, LANES), 0)
    lane = lax.broadcasted_iota(I32, (8, LANES), 1)
    return sub, lane, (sub + lane) % 2 == 0


def srl(x, n):
    return lax.shift_right_logical(x, jnp.full(x.shape, n, I32))


def up_one(x):
    return pltpu.roll(x, 7, 0)


def split_colours(first, second, even):
    moved = up_one(second)
    return jnp.where(even, first, moved), jnp.where(even, moved, first)


def transpose_bits(words, low_half=False):
    a = list(words)
    masks = {16: 0x0000FFFF, 8: 0x00FF00FF, 4: 0x0F0F0F0F, 2: 0x33333333, 1: 0x55555555}
    for j in (16, 8, 4, 2, 1):
        m = jnp.int32(masks[j])
        for k in range(32):
            if k & j:
                continue
            if low_half and j == 16:
                a[k], a[k + j] = a[k] & m, srl(a[k], 16)
                continue
            t = (srl(a[k], j) ^ a[k + j]) & m
            a[k + j] = a[k + j] ^ t
            a[k] = a[k] ^ (t << j)
    return a


def pack_spins(load):
    word = srl(load(0), 1) & 1
    for g in range(1, GROUPS):
        bit = 1 << g if g < 31 else -(1 << 31)
        word = word | (load(g) & jnp.int32(bit))
    return word


def own_kernel(thresholds, lattice, draws, planes, words, table):
    _, _, even = iotas()

    for b in range(8):
        r = [-(((thresholds[LEVELS - 1 - k] - 1) >> b) & 1) for k in range(LEVELS)]
        forms = (r[0], r[0] ^ r[1], r[0] ^ r[2], r[0] ^ r[1] ^ r[2] ^ r[3], r[0] ^ r[4])
        for n, form in enumerate(forms):
            table[b, n] = jnp.full((8, LANES), form, I32)

    def tile(ref, row, g):
        return ref[pl.ds(row, 8), pl.ds(g * LANES, LANES)]

    for q in range(2):
        first = pack_spins(lambda g: tile(lattice, 16 * q, g))
        second = pack_spins(lambda g: tile(lattice, 16 * q + 8, g))
        words[q, 0], words[q, 1] = split_colours(first, second, even)

    def body(n, carry):
        q, p = n // 2, n % 2
        row = pl.multiple_of(q * 16, 16)
        pairs = []
        for g in range(GROUPS):
            cols = pl.ds(g * LANES, LANES)
            pairs.append(split_colours(draws[p, pl.ds(row, 8), cols], draws[p, pl.ds(row + 8, 8), cols], even))
        for c in range(2):
            for b, plane in enumerate(transpose_bits([pair[c] for pair in pairs])):
                planes[q, c, p, b] = plane
        return carry

    lax.fori_loop(0, 4, body, 0)


def sweep_kernel(
    top, bot, from_partner, from_other, words, planes, table, final, means, edge0, edge1, side
):
    sub, lane, even = iotas()
    odd = jnp.logical_not(even)

    def tile(ref, row, g):
        return ref[pl.ds(row, 8), pl.ds(g * LANES, LANES)]

    def side_tile(q, n, half):
        if q in (0, 3):
            ref = bot if q == 3 or (n == 2 and half == 0) else top
            return tile(ref, (0, 16, 32)[n] + (8 * half if n < 2 else 0), GROUPS)
        return join_side(from_partner, from_other, 32 * n + 16 * (q - 1) + 8 * half)

    state = [[None] * 5, [None] * 5]
    for q, ref in ((0, top), (3, bot)):
        first = pack_spins(lambda g: tile(ref, 0, g))
        second = pack_spins(lambda g: tile(ref, 8, g))
        state[0][q], state[1][q] = split_colours(first, second, even)
    for q in (1, 2):
        for c in range(2):
            state[c][q] = words[q - 1, c]
    state[0][4] = state[1][4] = jnp.zeros((8, LANES), I32)
    for q in range(4):
        pair = split_colours(side_tile(q, 0, 0), side_tile(q, 0, 1), even)
        for c in range(2):
            state[c][4] = state[c][4] | ((srl(pair[c], 1) & 1) << q)

    for n, ref in enumerate((top, bot)):
        pairs = [split_colours(tile(ref, 16, g), tile(ref, 24, g), even) for g in range(GROUPS)]
        for c in range(2):
            for b, plane in enumerate(transpose_bits([pair[c] for pair in pairs])):
                edge0[n, c, b] = plane
    pairs = [split_colours(tile(bot, 32, g), tile(top, 32, g), even) for g in range(GROUPS)]
    for c in range(2):
        for b, plane in enumerate(transpose_bits([pair[c] for pair in pairs])):
            edge1[c, b] = plane
    slots = [jnp.zeros((8, LANES), I32)] * 32
    for q in range(4):
        slots[q], slots[4 + q] = split_colours(side_tile(q, 1, 0), side_tile(q, 1, 1), even)
        if q in (0, 3):
            slots[8 + q], slots[12 + q] = split_colours(side_tile(3, 2, 0), side_tile(0, 2, 1), even)
        else:
            slots[8 + q], slots[12 + q] = split_colours(side_tile(q, 2, 0), side_tile(q, 2, 1), even)
    for b, plane in enumerate(transpose_bits(slots, low_half=True)):
        side[b] = plane

    at_left, at_right = lane == 0, lane == LANES - 1
    fix = []
    for c in range(2):
        here, there = (even, odd) if c == 0 else (odd, even)
        fix.append(
            (here & (sub == 0), there & (sub == 7), here & (sub == 7), there & (sub == 6))
        )

    def half_sweep(mine, other, c, draw):
        up_prev, up_self, down_self, down_next = fix[c]
        left = [pltpu.roll(w, 1, 1) for w in other]
        right = [pltpu.roll(w, LANES - 1, 1) for w in other]
        side_left = srl(left[0], 31)
        side_right = right[0] & 1
        for q in range(1, 4):
            side_left = side_left | (srl(left[q], 31) << q)
            side_right = side_right | ((right[q] & 1) << q)
        new = []
        for q in range(5):
            w = other[q]
            if q < 4:
                from_side = srl(left[4], q) & 1
                lft = jnp.where(at_left, (left[q] << 1) | from_side, left[q])
                from_side = (right[4] << (31 - q)) & jnp.int32(-(1 << 31))
                rgt = jnp.where(at_right, srl(right[q], 1) | from_side, right[q])
                before = pltpu.roll(other[max(q - 1, 0)], 2, 0)
                after = pltpu.roll(other[min(q + 1, 3)], 6, 0)
            else:
                lft = jnp.where(at_left, side_left, left[4])
                rgt = jnp.where(at_right, side_right, right[4])
                before = pltpu.roll(w, 2, 0) << 1
                after = srl(pltpu.roll(w, 6, 0), 1)
            up = jnp.where(up_prev, before, jnp.where(up_self, w, pltpu.roll(w, 1, 0)))
            down = jnp.where(down_next, after, jnp.where(down_self, w, pltpu.roll(w, 7, 0)))
            s = mine[q]
            lft, rgt, up, down = lft ^ s, rgt ^ s, up ^ s, down ^ s
            s1, c1 = lft ^ rgt, lft & rgt
            s2, c2 = up ^ down, up & down
            k0 = s1 ^ s2
            k1 = (c1 ^ c2) | (s1 & s2)
            k2 = c1 & c2
            k01 = k0 & k1
            above = None
            for b in range(8):
                x = [table[b, n] for n in range(LEVELS)]
                limit = x[0] ^ (k0 & x[1]) ^ (k1 & x[2]) ^ (k01 & x[3]) ^ (k2 & x[4])
                u = draw(q, b)
                above = u & ~limit if above is None else above ^ ((u ^ limit) & (above ^ u))
            new.append(~(s ^ above))
        return new

    def sweep(p, t, a, b):
        def draw(c):
            def plane(q, bit):
                at = 8 * t + bit
                if q == 4:
                    return srl(side[at], 8 * p + 4 * c)
                if q in (1, 2):
                    return planes[q - 1, c, p, at]
                return edge0[q // 3, c, at] if p == 0 else edge1[c, at]

            return plane

        a = half_sweep(a, b, 0, draw(0))
        b = half_sweep(b, a, 1, draw(1))
        return a, b

    a, b = state
    for p in range(2):
        a, b = lax.fori_loop(0, 4, lambda t, ab: sweep(p, t, *ab), (a, b))

    sums = jnp.zeros((8, LANES), jnp.float32)
    for q in (1, 2):
        first = jnp.where(even, a[q], b[q])
        moved = jnp.where(even, b[q], a[q])
        second = pltpu.roll(moved, 1, 0)
        for n, word in enumerate((first, second)):
            row = 16 * (q - 1) + 8 * n
            minus = jnp.sum(lax.population_count(word).astype(jnp.float32), axis=1, keepdims=True)
            mean = (GROUPS * LANES - 2.0 * minus) * (1.0 / (4 * GROUPS * LANES))
            sums = sums + jnp.where(lane == row + sub, mean, 0.0)
            for g in range(GROUPS):
                spin = ((word << (31 - g)) >> 31) | 1
                final[pl.ds(row, 8), pl.ds(g * LANES, LANES)] = spin
    means[...] = jnp.sum(sums, axis=0, keepdims=True)[:, :32]


def side_kernel(lattice, draws, to_partner, to_other, sem):
    even = lax.axis_index("cols") % 2 == 0
    last = (GROUPS - 1) * LANES
    copies = []
    for target, column in ((to_partner, jnp.where(even, last, 0)), (to_other, jnp.where(even, 0, last))):
        at = pl.ds(pl.multiple_of(column, LANES), LANES)
        for n, ref in enumerate((lattice, draws.at[0], draws.at[1])):
            copies.append(pltpu.make_async_copy(ref.at[:, at], target.at[pl.ds(32 * n, 32), :], sem.at[len(copies)]))
    for copy in copies:
        copy.start()
    for copy in copies:
        copy.wait()


def join_side(from_partner, from_other, at):
    lane = lax.broadcasted_iota(I32, (8, LANES), 1)
    low = (lane < LANES // 2) == (lax.axis_index("cols") % 2 == 0)
    return jnp.where(low, from_partner[pl.ds(at, 8), :], from_other[pl.ds(at, 8), :])


def rows_kernel(lattice, draws, from_partner, from_other, down, up):
    for target, parts in (
        (down, ((0, 16, 16, 0), (1, 16, 16, 16), (2, 24, 8, 32))),
        (up, ((0, 0, 16, 0), (1, 0, 16, 16), (2, 0, 8, 32))),
    ):
        for n, row, rows, at in parts:
            ref = lattice if n == 0 else draws.at[n - 1]
            target[pl.ds(at, rows), pl.ds(0, GROUPS * LANES)] = ref[pl.ds(row, rows), :]
            for r in range(0, rows, 8):
                target[pl.ds(at + r, 8), pl.ds(GROUPS * LANES, LANES)] = join_side(
                    from_partner, from_other, 32 * n + row + r
                )


def shift(x, axis, by):
    count = lax.axis_size(axis)
    return lax.ppermute(x, axis, [(i, (i + by) % count) for i in range(count)])


def swap(x, axis, first):
    count = lax.axis_size(axis)
    pairs = [(i, (i + 1) % count) for i in range(first, count, 2)]
    return lax.ppermute(x, axis, pairs + [(j, i) for i, j in pairs])


def compiler_params():
    return pltpu.CompilerParams(vmem_limit_bytes=16 << 20)


def on_device(lattice, draws, thresholds):
    width = GROUPS * LANES
    vmem, smem = pl.BlockSpec(memory_space=pltpu.VMEM), pl.BlockSpec(memory_space=pltpu.SMEM)
    hbm = pl.BlockSpec(memory_space=pltpu.HBM)
    side = jax.ShapeDtypeStruct((96, LANES), I32)
    to_partner, to_other = pl.pallas_call(
        side_kernel,
        out_shape=(side, side),
        in_specs=[hbm] * 2,
        out_specs=(vmem,) * 2,
        scratch_shapes=[pltpu.SemaphoreType.DMA((6,))],
        compiler_params=compiler_params(),
        cost_estimate=pl.CostEstimate(flops=100_000, bytes_accessed=200_000, transcendentals=0),
    )(pltpu.with_memory_space_constraint(lattice, pltpu.HBM), pltpu.with_memory_space_constraint(draws, pltpu.HBM))
    from_other = swap(to_other, "cols", 1)
    from_partner = swap(to_partner, "cols", 0)

    rows = jax.ShapeDtypeStruct((40, width + LANES), I32)
    down, up = pl.pallas_call(
        rows_kernel,
        out_shape=(rows, rows),
        compiler_params=compiler_params(),
        cost_estimate=pl.CostEstimate(flops=1_000_000, bytes_accessed=3_000_000, transcendentals=0),
    )(lattice, draws, from_partner, from_other)
    top = shift(down, "rows", 1)
    bot = shift(up, "rows", -1)

    planes, words, table = pl.pallas_call(
        own_kernel,
        out_shape=(
            jax.ShapeDtypeStruct((2, 2, 2, 32, 8, LANES), I32),
            jax.ShapeDtypeStruct((2, 2, 8, LANES), I32),
            jax.ShapeDtypeStruct((8, LEVELS, 8, LANES), I32),
        ),
        in_specs=[smem, vmem, vmem],
        compiler_params=compiler_params(),
        cost_estimate=pl.CostEstimate(flops=30_000_000, bytes_accessed=2_700_000, transcendentals=0),
    )(thresholds, lattice, draws)

    final, means = pl.pallas_call(
        sweep_kernel,
        out_shape=(
            jax.ShapeDtypeStruct((32, width), I32),
            jax.ShapeDtypeStruct((1, 32), jnp.float32),
        ),
        in_specs=[vmem] * 7,
        scratch_shapes=[
            pltpu.VMEM((2, 2, 32, 8, LANES), I32),
            pltpu.VMEM((2, 32, 8, LANES), I32),
            pltpu.VMEM((32, 8, LANES), I32),
        ],
        compiler_params=compiler_params(),
        cost_estimate=pl.CostEstimate(flops=40_000_000, bytes_accessed=2_700_000, transcendentals=0),
    )(top, bot, from_partner, from_other, words, planes, table)
    return final, lax.psum(means, "cols").reshape(32)


def solution(mesh):
    in_specs = (P("rows", "cols"), P(None, "rows", "cols"), P())
    out_specs = (P("rows", "cols"), P("rows"))
    return jax.shard_map(
        on_device, mesh=mesh, in_specs=in_specs, out_specs=out_specs, check_vma=False
    )
```

```python
import jax
import jax.numpy as jnp
from jax import lax
from jax.experimental import pallas as pl
from jax.experimental.pallas import tpu as pltpu
from jax.sharding import PartitionSpec as P


SWEEPS = 8
LEVELS = 5
GROUPS = 32
LANES = 128
I32 = jnp.int32


def iotas():
    sub = lax.broadcasted_iota(I32, (8, LANES), 0)
    lane = lax.broadcasted_iota(I32, (8, LANES), 1)
    return sub, lane, (sub + lane) % 2 == 0


def srl(x, n):
    return lax.shift_right_logical(x, jnp.full(x.shape, n, I32))


def up_one(x):
    return pltpu.roll(x, 7, 0)


def split_colours(first, second, even):
    moved = up_one(second)
    return jnp.where(even, first, moved), jnp.where(even, moved, first)


def transpose_bits(words, low_half=False):
    a = list(words)
    masks = {16: 0x0000FFFF, 8: 0x00FF00FF, 4: 0x0F0F0F0F, 2: 0x33333333, 1: 0x55555555}
    for j in (16, 8, 4, 2, 1):
        m = jnp.int32(masks[j])
        for k in range(32):
            if k & j:
                continue
            if low_half and j == 16:
                a[k], a[k + j] = a[k] & m, srl(a[k], 16)
                continue
            t = (srl(a[k], j) ^ a[k + j]) & m
            a[k + j] = a[k + j] ^ t
            a[k] = a[k] ^ (t << j)
    return a


def pack_spins(load):
    word = srl(load(0), 1) & 1
    for g in range(1, GROUPS):
        bit = 1 << g if g < 31 else -(1 << 31)
        word = word | (load(g) & jnp.int32(bit))
    return word


def own_kernel(thresholds, lattice, draws, accept, words, table, planes, clears):
    _, _, even = iotas()

    bits = [[-(((thresholds[LEVELS - 1 - k] - 1) >> b) & 1) for b in range(8)] for k in range(LEVELS)]
    for b in range(8):
        r = [bits[k][b] for k in range(LEVELS)]
        forms = (r[0], r[0] ^ r[1], r[0] ^ r[2], r[0] ^ r[1] ^ r[2] ^ r[3], r[0] ^ r[4])
        for n, form in enumerate(forms):
            table[b, n] = jnp.full((8, LANES), form, I32)
        for k in range(LEVELS):
            clears[b, k] = jnp.full((8, LANES), ~bits[k][b], I32)

    def tile(ref, row, g):
        return ref[pl.ds(row, 8), pl.ds(g * LANES, LANES)]

    for q in range(2):
        first = pack_spins(lambda g: tile(lattice, 16 * q, g))
        second = pack_spins(lambda g: tile(lattice, 16 * q + 8, g))
        words[q, 0], words[q, 1] = split_colours(first, second, even)

    def body(n, carry):
        q, c, p = n // 4, n // 2 % 2, n % 2
        row = pl.multiple_of(q * 16, 16)
        mine = even == (c == 0)
        inputs = []
        for g in range(GROUPS):
            cols = pl.ds(g * LANES, LANES)
            inputs.append(jnp.where(mine, draws[p, pl.ds(row, 8), cols], up_one(draws[p, pl.ds(row + 8, 8), cols])))
        for b, plane in enumerate(transpose_bits(inputs)):
            planes[b] = plane

        def one_sweep(t, carry):
            u = [planes[8 * t + b] for b in range(8)]
            below = []
            for k in range(LEVELS):
                clear = [clears[b, k] for b in range(8)]
                z = clear[0]
                for b in range(8):
                    z = z & (u[b] ^ clear[b])
                    z = ~(z ^ clear[b]) if b == 7 else z ^ (clear[b] ^ clear[b + 1])
                below.append(z)
            r = below
            at = 4 * p + t
            accept[q, c, at, 0] = r[0]
            accept[q, c, at, 1] = r[0] ^ r[1]
            accept[q, c, at, 2] = r[0] ^ r[2]
            accept[q, c, at, 3] = r[0] ^ r[1] ^ r[2] ^ r[3]
            accept[q, c, at, 4] = r[0] ^ r[4]
            return carry

        return lax.fori_loop(0, 4, one_sweep, carry)

    lax.fori_loop(0, 8, body, 0)


def sweep_kernel(
    near, far, side, words, accept, table, final, means, edge0, edge1, side_planes, spins, sems
):
    sub, lane, even = iotas()
    odd = jnp.logical_not(even)

    def tile(ref, row, g):
        return ref[pl.ds(row, 8), pl.ds(g * LANES, LANES)]

    rows_even = rows_are_even()

    def edge_tile(q, row, g):
        at_near, at_far = tile(near, row, g), tile(far, row, g)
        return jnp.where(rows_even, at_far, at_near) if q == 0 else jnp.where(rows_even, at_near, at_far)

    def side_tile(q, n, half):
        if q in (0, 3):
            return edge_tile(q, (0, 16, 32)[n] + (8 * half if n < 2 else 0), GROUPS)
        return side[pl.ds(32 * n + 16 * (q - 1) + 8 * half, 8), :]

    state = [[None] * 5, [None] * 5]
    edges = []
    for ref in (near, far):
        first = pack_spins(lambda g: tile(ref, 0, g))
        second = pack_spins(lambda g: tile(ref, 8, g))
        edges.append(split_colours(first, second, even))
    for c in range(2):
        state[c][0] = jnp.where(rows_even, edges[1][c], edges[0][c])
        state[c][3] = jnp.where(rows_even, edges[0][c], edges[1][c])
    for q in (1, 2):
        for c in range(2):
            state[c][q] = words[q - 1, c]
    state[0][4] = state[1][4] = jnp.zeros((8, LANES), I32)
    for q in range(4):
        pair = split_colours(side_tile(q, 0, 0), side_tile(q, 0, 1), even)
        for c in range(2):
            state[c][4] = state[c][4] | ((srl(pair[c], 1) & 1) << q)

    for n, ref in enumerate((near, far)):
        pairs = [split_colours(tile(ref, 16, g), tile(ref, 24, g), even) for g in range(GROUPS)]
        for c in range(2):
            for b, plane in enumerate(transpose_bits([pair[c] for pair in pairs])):
                edge0[n, c, b] = plane
    pairs = [split_colours(edge_tile(3, 32, g), edge_tile(0, 32, g), even) for g in range(GROUPS)]
    for c in range(2):
        for b, plane in enumerate(transpose_bits([pair[c] for pair in pairs])):
            edge1[c, b] = plane
    slots = [jnp.zeros((8, LANES), I32)] * 32
    for q in range(4):
        slots[q], slots[4 + q] = split_colours(side_tile(q, 1, 0), side_tile(q, 1, 1), even)
        if q in (0, 3):
            slots[8 + q], slots[12 + q] = split_colours(side_tile(3, 2, 0), side_tile(0, 2, 1), even)
        else:
            slots[8 + q], slots[12 + q] = split_colours(side_tile(q, 2, 0), side_tile(q, 2, 1), even)
    for b, plane in enumerate(transpose_bits(slots, low_half=True)):
        side_planes[b] = plane

    at_left, at_right = lane == 0, lane == LANES - 1
    fix = []
    for c in range(2):
        here, there = (even, odd) if c == 0 else (odd, even)
        fix.append((here & (sub == 0), there & (sub == 7), here & (sub == 7), there & (sub == 6)))

    edge_at = {0: jnp.where(rows_even, 1, 0), 3: jnp.where(rows_even, 0, 1)}

    def half_sweep(mine, other, c, t):
        p, at = t // 4, t % 4
        joined = p == 1
        blocks = (0, 1, 2, 4) if joined else (0, 1, 2, 3, 4)
        up_prev, up_self, down_self, down_next = fix[c]
        left = {q: pltpu.roll(other[q], 1, 1) for q in blocks}
        right = {q: pltpu.roll(other[q], LANES - 1, 1) for q in blocks}
        side_left = jnp.zeros((8, LANES), I32)
        side_right = jnp.zeros((8, LANES), I32)
        for q in blocks[:-1]:
            if joined and q == 0:
                side_left = side_left | (srl(left[0], 31) * 9)
                side_right = side_right | ((right[0] & 1) * 9)
            else:
                side_left = side_left | (srl(left[q], 31) << q)
                side_right = side_right | ((right[q] & 1) << q)
        mine_first = even if c == 0 else odd
        new = {}
        for q in blocks:
            w, s = other[q], mine[q]
            if q < 4:
                if joined and q == 0:
                    from_left = jnp.where(mine_first, srl(left[4], 3), left[4]) & 1
                    from_right = jnp.where(mine_first, right[4] << 28, right[4] << 31) & jnp.int32(-(1 << 31))
                    before, after = other[2], other[1]
                else:
                    from_left = srl(left[4], q) & 1
                    from_right = (right[4] << (31 - q)) & jnp.int32(-(1 << 31))
                    before = other[max(q - 1, 0)]
                    after = other[0 if joined and q == 2 else min(q + 1, 3)]
                lft = jnp.where(at_left, (left[q] << 1) | from_left, left[q])
                rgt = jnp.where(at_right, srl(right[q], 1) | from_right, right[q])
                before, after = pltpu.roll(before, 2, 0), pltpu.roll(after, 6, 0)
            else:
                lft = jnp.where(at_left, side_left, left[4])
                rgt = jnp.where(at_right, side_right, right[4])
                before = pltpu.roll(w, 2, 0) << 1
                after = srl(pltpu.roll(w, 6, 0), 1)
            up = jnp.where(up_prev, before, jnp.where(up_self, w, pltpu.roll(w, 1, 0)))
            down = jnp.where(down_next, after, jnp.where(down_self, w, pltpu.roll(w, 7, 0)))
            lft, rgt, up, down = lft ^ s, rgt ^ s, up ^ s, down ^ s
            s1, c1 = lft ^ rgt, lft & rgt
            s2, c2 = up ^ down, up & down
            k0 = s1 ^ s2
            k1 = (c1 ^ c2) | (s1 & s2)
            k2 = c1 & c2
            k01 = k0 & k1
            if q in (1, 2):
                x = [accept[q - 1, c, t, n] for n in range(LEVELS)]
                flip = x[0] ^ (k0 & x[1]) ^ (k1 & x[2]) ^ (k01 & x[3]) ^ (k2 & x[4])
                new[q] = s ^ flip
                continue
            above = None
            for b in range(8):
                x = [table[b, n] for n in range(LEVELS)]
                limit = x[0] ^ (k0 & x[1]) ^ (k1 & x[2]) ^ (k01 & x[3]) ^ (k2 & x[4])
                if q == 4:
                    u = srl(side_planes[8 * at + b], 8 * p + 4 * c)
                elif joined:
                    u = edge1[c, 8 * at + b]
                else:
                    u = edge0[edge_at[q], c, 8 * at + b]
                above = u & ~limit if above is None else above ^ ((u ^ limit) & (above ^ u))
            new[q] = ~(s ^ above)
        return new

    a, b = ({q: colour[q] for q in range(5)} for colour in state)
    for t in range(SWEEPS):
        if t == 4:
            a[0] = jnp.where(even, a[3], a[0])
            b[0] = jnp.where(odd, b[3], b[0])
        a = half_sweep(a, b, 0, t)
        b = half_sweep(b, a, 1, t)

    copies = []
    tiles = []
    for q in (1, 2):
        first = jnp.where(even, a[q], b[q])
        second = pltpu.roll(jnp.where(even, b[q], a[q]), 1, 0)
        for n, word in enumerate((first, second)):
            row = 16 * (q - 1) + 8 * n
            for g in range(GROUPS):
                spins[pl.ds(row, 8), pl.ds(g * LANES, LANES)] = ((word << (31 - g)) >> 31) | 1
            at = pl.ds(row, 8)
            copies.append(pltpu.make_async_copy(spins.at[at], final.at[at], sems.at[len(copies)]))
            copies[-1].start()
            tiles.append((row, word))
    sums = jnp.zeros((8, LANES), jnp.float32)
    for row, word in tiles:
        minus = jnp.sum(lax.population_count(word).astype(jnp.float32), axis=1, keepdims=True)
        mean = (GROUPS * LANES - 2.0 * minus) * (1.0 / (4 * GROUPS * LANES))
        sums = sums + jnp.where(lane == row + sub, mean, 0.0)
    means[...] = jnp.sum(sums, axis=0, keepdims=True)[:, :32]
    for copy in copies:
        copy.wait()


def rows_are_even():
    return lax.axis_index("rows") % 2 == 0


def cols_are_even():
    return lax.axis_index("cols") % 2 == 0


def side_kernel(lattice, draws, to_partner, to_other, tiles, sem):
    lane = lax.broadcasted_iota(I32, (8, LANES), 1)
    last = (GROUPS - 1) * LANES
    copies = []
    for side, is_last in enumerate((jnp.logical_not(cols_are_even()), cols_are_even())):
        column = pl.ds(pl.multiple_of(jnp.where(is_last, last, 0), LANES), LANES)
        for n, ref in enumerate((lattice, draws.at[0], draws.at[1])):
            target = tiles.at[side, pl.ds(32 * n, 32), :]
            copies.append(pltpu.make_async_copy(ref.at[:, column], target, sem.at[len(copies)]))
            copies[-1].start()
    for copy in copies:
        copy.wait()
    for side, target, is_last in ((0, to_other, jnp.logical_not(cols_are_even())), (1, to_partner, cols_are_even())):
        skip = jnp.where(is_last, 16, 0)
        packed = [jnp.zeros((8, LANES), I32)] * 2
        for k in range(12):
            moved = pltpu.roll(tiles[side, pl.ds(8 * k, 8), :], (16 * (k % 8) + skip) % LANES, 1)
            packed[k // 8] = jnp.where(lane // 16 == k % 8, moved, packed[k // 8])
        target[pl.ds(0, 8), :], target[pl.ds(8, 8), :] = packed


def rows_kernel(lattice, draws, from_partner, from_other, side, near, far):
    lane = lax.broadcasted_iota(I32, (8, LANES), 1)
    partner_is_right = cols_are_even()
    low = (lane < LANES // 2) == partner_is_right
    for k in range(12):
        at = pl.ds(8 * (k // 8), 8)
        back = LANES - 16 * (k % 8)
        partner = pltpu.roll(from_partner[at, :], (back + jnp.where(partner_is_right, 0, LANES - 16)) % LANES, 1)
        other = pltpu.roll(from_other[at, :], (back + jnp.where(partner_is_right, LANES - 16, 0)) % LANES, 1)
        side[pl.ds(8 * k, 8), :] = jnp.where(low, partner, other)
    inner = pl.ds(0, GROUPS * LANES)
    outer = pl.ds(GROUPS * LANES, LANES)
    for target, down in ((far, jnp.logical_not(rows_are_even())), (near, rows_are_even())):
        for n, rows, at in ((0, 16, 0), (1, 16, 16), (2, 8, 32)):
            row = pl.multiple_of(jnp.where(down, 32 - rows, 0), 8)
            ref = lattice if n == 0 else draws.at[n - 1]
            target[pl.ds(at, rows), inner] = ref[pl.ds(row, rows), :]
            target[pl.ds(at, rows), outer] = side[pl.ds(pl.multiple_of(32 * n + row, 8), rows), :]


def swap(x, axis, first):
    count = lax.axis_size(axis)
    pairs = [(i, (i + 1) % count) for i in range(first, count, 2)]
    return lax.ppermute(x, axis, pairs + [(j, i) for i, j in pairs])


def on_device(lattice, draws, thresholds):
    width = GROUPS * LANES
    vmem, smem = pl.BlockSpec(memory_space=pltpu.VMEM), pl.BlockSpec(memory_space=pltpu.SMEM)

    def call(kernel, out_shape, flops, args, **kwargs):
        return pl.pallas_call(
            kernel,
            out_shape=out_shape,
            compiler_params=pltpu.CompilerParams(vmem_limit_bytes=16 << 20),
            cost_estimate=pl.CostEstimate(flops=flops, bytes_accessed=2_000_000, transcendentals=0),
            **kwargs,
        )(*args)

    def words(*shape):
        return jax.ShapeDtypeStruct(shape, I32)

    to_partner, to_other = call(
        side_kernel,
        (words(16, LANES),) * 2,
        1_000_000,
        tuple(pltpu.with_memory_space_constraint(x, pltpu.HBM) for x in (lattice, draws)),
        in_specs=[pl.BlockSpec(memory_space=pltpu.HBM)] * 2,
        scratch_shapes=[pltpu.VMEM((2, 96, LANES), I32), pltpu.SemaphoreType.DMA((6,))],
    )
    from_other = swap(to_other, "cols", 1)
    from_partner = swap(to_partner, "cols", 0)

    side, to_near, to_far = call(
        rows_kernel,
        (words(96, LANES), words(40, width + LANES), words(40, width + LANES)),
        1_000_000,
        (lattice, draws, from_partner, from_other),
    )
    far = swap(to_far, "rows", 1)
    near = swap(to_near, "rows", 0)

    accept, spins, table = call(
        own_kernel,
        (words(2, 2, SWEEPS, LEVELS, 8, LANES), words(2, 2, 8, LANES), words(8, LEVELS, 8, LANES)),
        50_000_000,
        (thresholds, lattice, draws),
        in_specs=[smem, vmem, vmem],
        scratch_shapes=[pltpu.VMEM((32, 8, LANES), I32), pltpu.VMEM((8, LEVELS, 8, LANES), I32)],
    )

    final, means = call(
        sweep_kernel,
        (words(32, width), jax.ShapeDtypeStruct((1, 32), jnp.float32)),
        40_000_000,
        (near, far, side, spins, accept, table),
        in_specs=[vmem] * 6,
        out_specs=(pl.BlockSpec(memory_space=pltpu.HBM), vmem),
        scratch_shapes=[
            pltpu.VMEM((2, 2, 32, 8, LANES), I32),
            pltpu.VMEM((2, 32, 8, LANES), I32),
            pltpu.VMEM((32, 8, LANES), I32),
            pltpu.VMEM((32, width), I32),
            pltpu.SemaphoreType.DMA((4,)),
        ],
    )
    return final, lax.psum(means, "cols").reshape(32)


def solution(mesh):
    in_specs = (P("rows", "cols"), P(None, "rows", "cols"), P())
    out_specs = (P("rows", "cols"), P("rows"))

    return jax.shard_map(on_device, mesh=mesh, in_specs=in_specs, out_specs=out_specs, check_vma=False)
```

```python
import jax
import jax.numpy as jnp
from jax import lax
from jax.experimental import pallas as pl
from jax.experimental.pallas import tpu as pltpu
from jax.sharding import PartitionSpec as P


SWEEPS = 8
LEVELS = 5
GROUPS = 32
LANES = 128
I32 = jnp.int32


def iotas():
    sub = lax.broadcasted_iota(I32, (8, LANES), 0)
    lane = lax.broadcasted_iota(I32, (8, LANES), 1)
    return sub, lane, (sub + lane) % 2 == 0


def srl(x, n):
    return lax.shift_right_logical(x, jnp.full(x.shape, n, I32))


def up_one(x):
    return pltpu.roll(x, 7, 0)


def split_colours(first, second, even):
    moved = up_one(second)
    return jnp.where(even, first, moved), jnp.where(even, moved, first)


def transpose_bits(words, low_half=False):
    a = list(words)
    masks = {16: 0x0000FFFF, 8: 0x00FF00FF, 4: 0x0F0F0F0F, 2: 0x33333333, 1: 0x55555555}
    for j in (16, 8, 4, 2, 1):
        m = jnp.int32(masks[j])
        for k in range(32):
            if k & j:
                continue
            if low_half and j == 16:
                a[k], a[k + j] = a[k] & m, srl(a[k], 16)
                continue
            t = (srl(a[k], j) ^ a[k + j]) & m
            a[k + j] = a[k + j] ^ t
            a[k] = a[k] ^ (t << j)
    return a


def pack_spins(load):
    word = srl(load(0), 1) & 1
    for g in range(1, GROUPS):
        bit = 1 << g if g < 31 else -(1 << 31)
        word = word | (load(g) & jnp.int32(bit))
    return word


def own_kernel(thresholds, lattice, draws, accept, words, table, planes, clears):
    _, _, even = iotas()

    bits = [[-(((thresholds[LEVELS - 1 - k] - 1) >> b) & 1) for b in range(8)] for k in range(LEVELS)]
    for b in range(8):
        r = [bits[k][b] for k in range(LEVELS)]
        forms = (r[0], r[0] ^ r[1], r[0] ^ r[2], r[0] ^ r[1] ^ r[2] ^ r[3], r[0] ^ r[4])
        for n, form in enumerate(forms):
            table[b, n] = jnp.full((8, LANES), form, I32)
        for k in range(LEVELS):
            clears[b, k] = jnp.full((8, LANES), ~bits[k][b], I32)

    def tile(ref, row, g):
        return ref[pl.ds(row, 8), pl.ds(g * LANES, LANES)]

    for q in range(2):
        first = pack_spins(lambda g: tile(lattice, 16 * q, g))
        second = pack_spins(lambda g: tile(lattice, 16 * q + 8, g))
        words[q, 0], words[q, 1] = split_colours(first, second, even)

    def body(n, carry):
        q, c, p = n // 4, n // 2 % 2, n % 2
        row = pl.multiple_of(q * 16, 16)
        mine = even == (c == 0)
        inputs = []
        for g in range(GROUPS):
            cols = pl.ds(g * LANES, LANES)
            inputs.append(jnp.where(mine, draws[p, pl.ds(row, 8), cols], up_one(draws[p, pl.ds(row + 8, 8), cols])))
        for b, plane in enumerate(transpose_bits(inputs)):
            planes[b] = plane

        def one_sweep(t, carry):
            u = [planes[8 * t + b] for b in range(8)]
            below = []
            for k in range(LEVELS):
                clear = [clears[b, k] for b in range(8)]
                z = clear[0]
                for b in range(8):
                    z = z & (u[b] ^ clear[b])
                    z = ~(z ^ clear[b]) if b == 7 else z ^ (clear[b] ^ clear[b + 1])
                below.append(z)
            r = below
            at = 4 * p + t
            accept[q, c, at, 0] = r[0]
            accept[q, c, at, 1] = r[0] ^ r[1]
            accept[q, c, at, 2] = r[0] ^ r[2]
            accept[q, c, at, 3] = r[0] ^ r[1] ^ r[2] ^ r[3]
            accept[q, c, at, 4] = r[0] ^ r[4]
            return carry

        return lax.fori_loop(0, 4, one_sweep, carry)

    lax.fori_loop(0, 8, body, 0)


def sweep_kernel(
    near_top, near, far, side, words, accept, table, final, means, edge0, edge1, side_planes, packed, spins, sems
):
    sub, lane, even = iotas()
    odd = jnp.logical_not(even)

    def from_near(row):
        return near_top[pl.ds(row, 8), :] | near[pl.ds(row, 8), :]

    def from_far(row):
        return far[pl.ds(row, 8), :]

    def read_edges(top, bot):
        for n, load in enumerate((top, bot)):
            first = pack_spins(lambda g: load(DEEP * g))
            second = pack_spins(lambda g: load(DEEP * g + 8))
            packed[n, 0], packed[n, 1] = split_colours(first, second, even)
            at = 15 if n == 0 else 16
            pairs = [split_colours(load(DEEP * g + at), load(DEEP * g + at + 8), even) for g in range(GROUPS)]
            for c in range(2):
                for b, plane in enumerate(transpose_bits([pair[c] for pair in pairs])):
                    edge0[n, c, b] = plane
        pairs = [split_colours(bot(DEEP * g + 31), top(DEEP * g + 30), even) for g in range(GROUPS)]
        for c in range(2):
            for b, plane in enumerate(transpose_bits([pair[c] for pair in pairs])):
                edge1[c, b] = plane

        outer = []
        for load in (top, bot):
            dense = (load(SIDE_AT), load(SIDE_AT + 8))
            outer.append([pltpu.roll(dense[k // 4], LANES - 16 - 32 * (k % 4), 1) for k in range(4)])
            outer[-1].append(pltpu.roll(dense[1], LANES - 16, 1))

        def side_tiles(q, n):
            if q in (0, 3):
                return outer[q // 3][2 * n], outer[q // 3][2 * n + 1]
            at = 32 * n + 16 * (q - 1)
            return side[pl.ds(at, 8), :], side[pl.ds(at + 8, 8), :]

        columns = [jnp.zeros((8, LANES), I32)] * 2
        slots = [jnp.zeros((8, LANES), I32)] * 32
        for q in range(4):
            pair = split_colours(*side_tiles(q, 0), even)
            for c in range(2):
                columns[c] = columns[c] | ((srl(pair[c], 1) & 1) << q)
            slots[q], slots[4 + q] = split_colours(*side_tiles(q, 1), even)
            second_word = (outer[1][4], outer[0][4]) if q in (0, 3) else side_tiles(q, 2)
            slots[8 + q], slots[12 + q] = split_colours(*second_word, even)
        packed[2, 0], packed[2, 1] = columns
        for b, plane in enumerate(transpose_bits(slots, low_half=True)):
            side_planes[b] = plane

    @pl.when(rows_are_even())
    def _():
        read_edges(from_far, from_near)

    @pl.when(jnp.logical_not(rows_are_even()))
    def _():
        read_edges(from_near, from_far)

    state = [[packed[0, c], words[0, c], words[1, c], packed[1, c], packed[2, c]] for c in range(2)]

    at_left, at_right = lane == 0, lane == LANES - 1
    fix = []
    for c in range(2):
        here, there = (even, odd) if c == 0 else (odd, even)
        fix.append((here & (sub == 0), there & (sub == 7), here & (sub == 7), there & (sub == 6)))

    def half_sweep(mine, other, c, t):
        p, at = t // 4, t % 4
        joined = p == 1
        blocks = (0, 1, 2, 4) if joined else (0, 1, 2, 3, 4)
        up_prev, up_self, down_self, down_next = fix[c]
        left = {q: pltpu.roll(other[q], 1, 1) for q in blocks}
        right = {q: pltpu.roll(other[q], LANES - 1, 1) for q in blocks}
        side_left = jnp.zeros((8, LANES), I32)
        side_right = jnp.zeros((8, LANES), I32)
        for q in blocks[:-1]:
            if joined and q == 0:
                side_left = side_left | (srl(left[0], 31) * 9)
                side_right = side_right | ((right[0] & 1) * 9)
            else:
                side_left = side_left | (srl(left[q], 31) << q)
                side_right = side_right | ((right[q] & 1) << q)
        mine_first = even if c == 0 else odd
        new = {}
        for q in blocks:
            w, s = other[q], mine[q]
            if q < 4:
                if joined and q == 0:
                    from_left = jnp.where(mine_first, srl(left[4], 3), left[4]) & 1
                    from_right = jnp.where(mine_first, right[4] << 28, right[4] << 31) & jnp.int32(-(1 << 31))
                    before, after = other[2], other[1]
                else:
                    from_left = srl(left[4], q) & 1
                    from_right = (right[4] << (31 - q)) & jnp.int32(-(1 << 31))
                    before = other[max(q - 1, 0)]
                    after = other[0 if joined and q == 2 else min(q + 1, 3)]
                lft = jnp.where(at_left, (left[q] << 1) | from_left, left[q])
                rgt = jnp.where(at_right, srl(right[q], 1) | from_right, right[q])
                before, after = pltpu.roll(before, 2, 0), pltpu.roll(after, 6, 0)
            else:
                lft = jnp.where(at_left, side_left, left[4])
                rgt = jnp.where(at_right, side_right, right[4])
                before = pltpu.roll(w, 2, 0) << 1
                after = srl(pltpu.roll(w, 6, 0), 1)
            up = jnp.where(up_prev, before, jnp.where(up_self, w, pltpu.roll(w, 1, 0)))
            down = jnp.where(down_next, after, jnp.where(down_self, w, pltpu.roll(w, 7, 0)))
            lft, rgt, up, down = lft ^ s, rgt ^ s, up ^ s, down ^ s
            s1, c1 = lft ^ rgt, lft & rgt
            s2, c2 = up ^ down, up & down
            k0 = s1 ^ s2
            k1 = (c1 ^ c2) | (s1 & s2)
            k2 = c1 & c2
            k01 = k0 & k1
            if q in (1, 2):
                x = [accept[q - 1, c, t, n] for n in range(LEVELS)]
                flip = x[0] ^ (k0 & x[1]) ^ (k1 & x[2]) ^ (k01 & x[3]) ^ (k2 & x[4])
                new[q] = s ^ flip
                continue
            above = None
            for b in range(8):
                x = [table[b, n] for n in range(LEVELS)]
                limit = x[0] ^ (k0 & x[1]) ^ (k1 & x[2]) ^ (k01 & x[3]) ^ (k2 & x[4])
                if q == 4:
                    u = srl(side_planes[8 * at + b], 8 * p + 4 * c)
                elif joined:
                    u = edge1[c, 8 * at + b]
                else:
                    u = edge0[q // 3, c, 8 * at + b]
                above = u & ~limit if above is None else above ^ ((u ^ limit) & (above ^ u))
            new[q] = ~(s ^ above)
        return new

    a, b = ({q: colour[q] for q in range(5)} for colour in state)
    for t in range(SWEEPS):
        if t == 4:
            a[0] = jnp.where(even, a[3], a[0])
            b[0] = jnp.where(odd, b[3], b[0])
        a = half_sweep(a, b, 0, t)
        b = half_sweep(b, a, 1, t)

    copies = []
    tiles = []
    for q in (1, 2):
        first = jnp.where(even, a[q], b[q])
        second = pltpu.roll(jnp.where(even, b[q], a[q]), 1, 0)
        for n, word in enumerate((first, second)):
            row = 16 * (q - 1) + 8 * n
            for g in range(GROUPS):
                spins[pl.ds(row, 8), pl.ds(g * LANES, LANES)] = ((word << (31 - g)) >> 31) | 1
            at = pl.ds(row, 8)
            copies.append(pltpu.make_async_copy(spins.at[at], final.at[at], sems.at[len(copies)]))
            copies[-1].start()
            tiles.append((row, word))
    sums = jnp.zeros((8, LANES), jnp.float32)
    for row, word in tiles:
        minus = jnp.sum(lax.population_count(word).astype(jnp.float32), axis=1, keepdims=True)
        mean = (GROUPS * LANES - 2.0 * minus) * (1.0 / (4 * GROUPS * LANES))
        sums = sums + jnp.where(lane == row + sub, mean, 0.0)
    means[...] = jnp.sum(sums, axis=0, keepdims=True)[:, :32]
    for copy in copies:
        copy.wait()


def rows_are_even():
    return lax.axis_index("rows") % 2 == 0


def cols_are_even():
    return lax.axis_index("cols") % 2 == 0


def side_kernel(lattice, draws, to_partner, to_other, tiles, sem):
    lane = lax.broadcasted_iota(I32, (8, LANES), 1)
    last = (GROUPS - 1) * LANES
    copies = []
    for side, is_last in enumerate((jnp.logical_not(cols_are_even()), cols_are_even())):
        column = pl.ds(pl.multiple_of(jnp.where(is_last, last, 0), LANES), LANES)
        for n, ref in enumerate((lattice, draws.at[0], draws.at[1])):
            target = tiles.at[side, pl.ds(32 * n, 32), :]
            copies.append(pltpu.make_async_copy(ref.at[:, column], target, sem.at[len(copies)]))
            copies[-1].start()
    for copy in copies:
        copy.wait()
    for side, target, is_last in ((0, to_other, jnp.logical_not(cols_are_even())), (1, to_partner, cols_are_even())):
        skip = jnp.where(is_last, 16, 0)
        packed = [jnp.zeros((8, LANES), I32)] * 2
        for k in range(12):
            moved = pltpu.roll(tiles[side, pl.ds(8 * k, 8), :], (16 * (k % 8) + skip) % LANES, 1)
            packed[k // 8] = jnp.where(lane // 16 == k % 8, moved, packed[k // 8])
        target[pl.ds(0, 8), :], target[pl.ds(8, 8), :] = packed


DEEP = 38
SIDE_AT = DEEP * GROUPS
MESSAGE = SIDE_AT + 16


def rows_kernel(lattice, draws, from_partner, from_other, side, near, far):
    lane = lax.broadcasted_iota(I32, (8, LANES), 1)
    partner_is_right = cols_are_even()
    low = (lane < LANES // 2) == partner_is_right
    for k in range(12):
        at = pl.ds(8 * (k // 8), 8)
        back = LANES - 16 * (k % 8)
        partner = pltpu.roll(from_partner[at, :], (back + jnp.where(partner_is_right, 0, LANES - 16)) % LANES, 1)
        other = pltpu.roll(from_other[at, :], (back + jnp.where(partner_is_right, LANES - 16, 0)) % LANES, 1)
        side[pl.ds(8 * k, 8), :] = jnp.where(low, partner, other)

    def write(target, down):
        below = (((2, 24), 30), ((1, 24), 23), ((1, 16), 15), ((0, 24), 8), ((0, 16), 0))
        above = (((0, 0), 0), ((0, 8), 8), ((1, 0), 16), ((1, 8), 24), ((2, 0), 31))
        for g in range(GROUPS):
            for (n, row), at in below if down else above:
                ref = lattice if n == 0 else draws.at[n - 1]
                target[pl.ds(DEEP * g + at, 8), :] = ref[pl.ds(row, 8), pl.ds(g * LANES, LANES)]
        start = 16 if down else 0
        dense = jnp.zeros((8, LANES), I32)
        for k, row in enumerate((start, start + 8, 32 + start, 40 + start, 88 if down else 64)):
            moved = pltpu.roll(side[pl.ds(row, 8), :], (32 * (k % 4) + 16) % LANES, 1)
            dense = jnp.where(lane // 32 == k % 4, moved, dense)
            if k >= 3:
                target[pl.ds(SIDE_AT + 8 * (k - 3), 8), :] = dense

    @pl.when(rows_are_even())
    def _():
        write(near, True)
        write(far, False)

    @pl.when(jnp.logical_not(rows_are_even()))
    def _():
        write(far, True)
        write(near, False)


def swap(x, axis, first, only=None):
    count = lax.axis_size(axis)
    pairs = [(i, (i + 1) % count) for i in range(first, count, 2)][only or slice(None)]
    return lax.ppermute(x, axis, pairs + [(j, i) for i, j in pairs])


def on_device(lattice, draws, thresholds):
    width = GROUPS * LANES
    vmem, smem = pl.BlockSpec(memory_space=pltpu.VMEM), pl.BlockSpec(memory_space=pltpu.SMEM)

    def call(kernel, out_shape, flops, args, **kwargs):
        return pl.pallas_call(
            kernel,
            out_shape=out_shape,
            compiler_params=pltpu.CompilerParams(vmem_limit_bytes=16 << 20),
            cost_estimate=pl.CostEstimate(flops=flops, bytes_accessed=2_000_000, transcendentals=0),
            **kwargs,
        )(*args)

    def words(*shape):
        return jax.ShapeDtypeStruct(shape, I32)

    to_partner, to_other = call(
        side_kernel,
        (words(16, LANES),) * 2,
        1_000_000,
        tuple(pltpu.with_memory_space_constraint(x, pltpu.HBM) for x in (lattice, draws)),
        in_specs=[pl.BlockSpec(memory_space=pltpu.HBM)] * 2,
        scratch_shapes=[pltpu.VMEM((2, 96, LANES), I32), pltpu.SemaphoreType.DMA((6,))],
    )
    from_other = swap(to_other, "cols", 1)
    from_partner = swap(to_partner, "cols", 0)

    side, to_near, to_far = call(
        rows_kernel,
        (words(96, LANES), words(MESSAGE, LANES), words(MESSAGE, LANES)),
        1_000_000,
        (lattice, draws, from_partner, from_other),
    )
    near_top = swap(to_near, "rows", 0, slice(0, 1))
    far = swap(to_far, "rows", 1)
    near = swap(to_near, "rows", 0, slice(1, None))

    accept, spins, table = call(
        own_kernel,
        (words(2, 2, SWEEPS, LEVELS, 8, LANES), words(2, 2, 8, LANES), words(8, LEVELS, 8, LANES)),
        50_000_000,
        (thresholds, lattice, draws),
        in_specs=[smem, vmem, vmem],
        scratch_shapes=[pltpu.VMEM((32, 8, LANES), I32), pltpu.VMEM((8, LEVELS, 8, LANES), I32)],
    )

    final, means = call(
        sweep_kernel,
        (words(32, width), jax.ShapeDtypeStruct((1, 32), jnp.float32)),
        40_000_000,
        (near_top, near, far, side, spins, accept, table),
        in_specs=[vmem] * 7,
        out_specs=(pl.BlockSpec(memory_space=pltpu.HBM), vmem),
        scratch_shapes=[
            pltpu.VMEM((2, 2, 32, 8, LANES), I32),
            pltpu.VMEM((2, 32, 8, LANES), I32),
            pltpu.VMEM((32, 8, LANES), I32),
            pltpu.VMEM((3, 2, 8, LANES), I32),
            pltpu.VMEM((32, width), I32),
            pltpu.SemaphoreType.DMA((4,)),
        ],
    )
    return final, lax.psum(means, "cols").reshape(32)


def solution(mesh):
    in_specs = (P("rows", "cols"), P(None, "rows", "cols"), P())
    out_specs = (P("rows", "cols"), P("rows"))

    return jax.shard_map(on_device, mesh=mesh, in_specs=in_specs, out_specs=out_specs, check_vma=False)
```

```python
import jax
import jax.numpy as jnp
from jax import lax
from jax.experimental import pallas as pl
from jax.experimental.pallas import tpu as pltpu
from jax.sharding import PartitionSpec as P


SWEEPS = 8
LEVELS = 5
GROUPS = 32
LANES = 128
I32 = jnp.int32


def iotas():
    sub = lax.broadcasted_iota(I32, (8, LANES), 0)
    lane = lax.broadcasted_iota(I32, (8, LANES), 1)
    return sub, lane, (sub + lane) % 2 == 0


def srl(x, n):
    return lax.shift_right_logical(x, jnp.full(x.shape, n, I32))


def up_one(x):
    return pltpu.roll(x, 7, 0)


def split_colours(first, second, even):
    moved = up_one(second)
    return jnp.where(even, first, moved), jnp.where(even, moved, first)


def transpose_bits(words, low_half=False):
    a = list(words)
    masks = {16: 0x0000FFFF, 8: 0x00FF00FF, 4: 0x0F0F0F0F, 2: 0x33333333, 1: 0x55555555}
    for j in (16, 8, 4, 2, 1):
        m = jnp.int32(masks[j])
        for k in range(32):
            if k & j:
                continue
            if low_half and j == 16:
                a[k], a[k + j] = a[k] & m, srl(a[k], 16)
                continue
            t = (srl(a[k], j) ^ a[k + j]) & m
            a[k + j] = a[k + j] ^ t
            a[k] = a[k] ^ (t << j)
    return a


def pack_spins(load):
    word = srl(load(0), 1) & 1
    for g in range(1, GROUPS):
        bit = 1 << g if g < 31 else -(1 << 31)
        word = word | (load(g) & jnp.int32(bit))
    return word


def acceptance(u, table):
    r = []
    for k in range(LEVELS):
        z = table[0, 0, k]
        for b in range(8):
            z = (z & (u[b] ^ table[0, b, k])) ^ table[1, b, k]
        r.append(z)
    return r


def own_kernel(thresholds, lattice, draws, accept, words, table, planes):
    _, _, even = iotas()

    for k in range(LEVELS):
        clear = [((thresholds[LEVELS - 1 - k] - 1) >> b & 1) - 1 for b in range(8)]
        for b in range(8):
            table[0, b, k] = jnp.full((8, LANES), clear[b], I32)
            table[1, b, k] = jnp.full((8, LANES), clear[b] ^ (clear[b + 1] if b < 7 else -1), I32)

    def tile(ref, row, g):
        return ref[pl.ds(row, 8), pl.ds(g * LANES, LANES)]

    for q in range(2):
        first = pack_spins(lambda g: tile(lattice, 16 * q, g))
        second = pack_spins(lambda g: tile(lattice, 16 * q + 8, g))
        words[q, 0], words[q, 1] = split_colours(first, second, even)

    def body(n, carry):
        q, c, p = n // 4, n // 2 % 2, n % 2
        row = pl.multiple_of(q * 16, 16)
        mine = even == (c == 0)
        inputs = []
        for g in range(GROUPS):
            cols = pl.ds(g * LANES, LANES)
            inputs.append(jnp.where(mine, draws[p, pl.ds(row, 8), cols], up_one(draws[p, pl.ds(row + 8, 8), cols])))
        for b, plane in enumerate(transpose_bits(inputs)):
            planes[b] = plane

        def one_sweep(t, carry):
            u = [planes[8 * t + b] for b in range(8)]
            at = 4 * p + t
            for n, form in enumerate(acceptance(u, table)):
                accept[q, c, at, n] = form
            return carry

        return lax.fori_loop(0, 4, one_sweep, carry)

    lax.fori_loop(0, 8, body, 0)


def sweep_kernel(
    near_top, near, far, side, words, accept, table, final, means, edge0, edge1, side_planes, packed, spins, sems
):
    sub, lane, even = iotas()
    odd = jnp.logical_not(even)

    def from_near(row):
        return near_top[pl.ds(row, 8), :] | near[pl.ds(row, 8), :]

    def from_far(row):
        return far[pl.ds(row, 8), :]

    def read_edges(top, bot):
        for n, load in enumerate((top, bot)):
            first = pack_spins(lambda g: load(DEEP * g))
            second = pack_spins(lambda g: load(DEEP * g + 8))
            packed[n, 0], packed[n, 1] = split_colours(first, second, even)
            at = 15 if n == 0 else 16
            pairs = [split_colours(load(DEEP * g + at), load(DEEP * g + at + 8), even) for g in range(GROUPS)]
            for c in range(2):
                for b, plane in enumerate(transpose_bits([pair[c] for pair in pairs])):
                    edge0[n, c, b] = plane
        pairs = [split_colours(bot(DEEP * g + 31), top(DEEP * g + 30), even) for g in range(GROUPS)]
        for c in range(2):
            for b, plane in enumerate(transpose_bits([pair[c] for pair in pairs])):
                edge1[c, b] = plane

        outer = []
        for load in (top, bot):
            dense = (load(SIDE_AT), load(SIDE_AT + 8))
            outer.append([pltpu.roll(dense[k // 4], LANES - 16 - 32 * (k % 4), 1) for k in range(4)])
            outer[-1].append(pltpu.roll(dense[1], LANES - 16, 1))

        def side_tiles(q, n):
            if q in (0, 3):
                return outer[q // 3][2 * n], outer[q // 3][2 * n + 1]
            at = 32 * n + 16 * (q - 1)
            return side[pl.ds(at, 8), :], side[pl.ds(at + 8, 8), :]

        columns = [jnp.zeros((8, LANES), I32)] * 2
        slots = [jnp.zeros((8, LANES), I32)] * 32
        for q in range(4):
            pair = split_colours(*side_tiles(q, 0), even)
            for c in range(2):
                columns[c] = columns[c] | ((srl(pair[c], 1) & 1) << q)
            slots[q], slots[4 + q] = split_colours(*side_tiles(q, 1), even)
            second_word = (outer[1][4], outer[0][4]) if q in (0, 3) else side_tiles(q, 2)
            slots[8 + q], slots[12 + q] = split_colours(*second_word, even)
        packed[2, 0], packed[2, 1] = columns
        for b, plane in enumerate(transpose_bits(slots, low_half=True)):
            side_planes[b] = plane

    @pl.when(rows_are_even())
    def _():
        read_edges(from_far, from_near)

    @pl.when(jnp.logical_not(rows_are_even()))
    def _():
        read_edges(from_near, from_far)

    state = [[packed[0, c], words[0, c], words[1, c], packed[1, c], packed[2, c]] for c in range(2)]

    at_left, at_right = lane == 0, lane == LANES - 1
    fix = []
    for c in range(2):
        here, there = (even, odd) if c == 0 else (odd, even)
        fix.append((here & (sub == 0), there & (sub == 7), here & (sub == 7), there & (sub == 6)))

    def rules_of(c, t):
        p, at = t // 4, t % 4
        joined = p == 1
        blocks = (0, 1, 2, 4) if joined else (0, 1, 2, 3, 4)
        rules = {}
        for q in blocks:
            if q in (1, 2):
                rules[q] = [accept[q - 1, c, t, n] for n in range(LEVELS)]
                continue
            if q == 4:
                u = [srl(side_planes[8 * at + b], 8 * p + 4 * c) for b in range(8)]
            elif joined:
                u = [edge1[c, 8 * at + b] for b in range(8)]
            else:
                u = [edge0[q // 3, c, 8 * at + b] for b in range(8)]
            rules[q] = acceptance(u, table)
        return rules

    def half_sweep(mine, other, c, t, rules):
        p = t // 4
        joined = p == 1
        blocks = (0, 1, 2, 4) if joined else (0, 1, 2, 3, 4)
        up_prev, up_self, down_self, down_next = fix[c]
        left = {q: pltpu.roll(other[q], 1, 1) for q in blocks}
        right = {q: pltpu.roll(other[q], LANES - 1, 1) for q in blocks}
        side_left = jnp.zeros((8, LANES), I32)
        side_right = jnp.zeros((8, LANES), I32)
        for q in blocks[:-1]:
            if joined and q == 0:
                side_left = side_left | (srl(left[0], 31) * 9)
                side_right = side_right | ((right[0] & 1) * 9)
            else:
                side_left = side_left | (srl(left[q], 31) << q)
                side_right = side_right | ((right[q] & 1) << q)
        mine_first = even if c == 0 else odd
        new = {}
        for q in blocks:
            w, s = other[q], mine[q]
            if q < 4:
                if joined and q == 0:
                    from_left = jnp.where(mine_first, srl(left[4], 3), left[4]) & 1
                    from_right = jnp.where(mine_first, right[4] << 28, right[4] << 31) & jnp.int32(-(1 << 31))
                    before, after = other[2], other[1]
                else:
                    from_left = srl(left[4], q) & 1
                    from_right = (right[4] << (31 - q)) & jnp.int32(-(1 << 31))
                    before = other[max(q - 1, 0)]
                    after = other[0 if joined and q == 2 else min(q + 1, 3)]
                lft = jnp.where(at_left, (left[q] << 1) | from_left, left[q])
                rgt = jnp.where(at_right, srl(right[q], 1) | from_right, right[q])
                before, after = pltpu.roll(before, 2, 0), pltpu.roll(after, 6, 0)
            else:
                lft = jnp.where(at_left, side_left, left[4])
                rgt = jnp.where(at_right, side_right, right[4])
                before = pltpu.roll(w, 2, 0) << 1
                after = srl(pltpu.roll(w, 6, 0), 1)
            up = jnp.where(up_prev, before, jnp.where(up_self, w, pltpu.roll(w, 1, 0)))
            down = jnp.where(down_next, after, jnp.where(down_self, w, pltpu.roll(w, 7, 0)))
            lft, rgt, up, down = lft ^ s, rgt ^ s, up ^ s, down ^ s
            r = rules[q]
            one, two = up ^ down, up & down
            with_none = r[0] ^ (one & (r[0] ^ r[1])) ^ (two & (r[0] ^ r[2]))
            with_one = r[1] ^ (one & (r[1] ^ r[2])) ^ (two & (r[1] ^ r[3]))
            with_two = r[2] ^ (one & (r[2] ^ r[3])) ^ (two & (r[2] ^ r[4]))
            keep = s ^ with_none
            new[q] = keep ^ ((lft ^ rgt) & (with_none ^ with_one)) ^ ((lft & rgt) & (with_none ^ with_two))
        return new

    a, b = ({q: colour[q] for q in range(5)} for colour in state)
    rules = rules_of(0, 0)
    for t in range(SWEEPS):
        if t == 4:
            a[0] = jnp.where(even, a[3], a[0])
            b[0] = jnp.where(odd, b[3], b[0])
        after = rules_of(1, t)
        a = half_sweep(a, b, 0, t, rules)
        rules = rules_of(0, t + 1) if t < SWEEPS - 1 else None
        b = half_sweep(b, a, 1, t, after)

    copies = []
    tiles = []
    for q in (1, 2):
        first = jnp.where(even, a[q], b[q])
        second = pltpu.roll(jnp.where(even, b[q], a[q]), 1, 0)
        for n, word in enumerate((first, second)):
            row = 16 * (q - 1) + 8 * n
            for g in range(GROUPS):
                spins[pl.ds(row, 8), pl.ds(g * LANES, LANES)] = ((word << (31 - g)) >> 31) | 1
            at = pl.ds(row, 8)
            copies.append(pltpu.make_async_copy(spins.at[at], final.at[at], sems.at[len(copies)]))
            copies[-1].start()
            tiles.append((row, word))
    sums = jnp.zeros((8, LANES), jnp.float32)
    for row, word in tiles:
        minus = jnp.sum(lax.population_count(word).astype(jnp.float32), axis=1, keepdims=True)
        mean = (GROUPS * LANES - 2.0 * minus) * (1.0 / (4 * GROUPS * LANES))
        sums = sums + jnp.where(lane == row + sub, mean, 0.0)
    means[...] = jnp.sum(sums, axis=0, keepdims=True)[:, :32]
    for copy in copies:
        copy.wait()


def rows_are_even():
    return lax.axis_index("rows") % 2 == 0


def cols_are_even():
    return lax.axis_index("cols") % 2 == 0


def side_kernel(lattice, draws, to_partner, to_other, tiles, sem):
    lane = lax.broadcasted_iota(I32, (8, LANES), 1)
    last = (GROUPS - 1) * LANES
    copies = []
    for side, is_last in enumerate((jnp.logical_not(cols_are_even()), cols_are_even())):
        column = pl.ds(pl.multiple_of(jnp.where(is_last, last, 0), LANES), LANES)
        for n, ref in enumerate((lattice, draws.at[0], draws.at[1])):
            target = tiles.at[side, pl.ds(32 * n, 32), :]
            copies.append(pltpu.make_async_copy(ref.at[:, column], target, sem.at[len(copies)]))
            copies[-1].start()
    for copy in copies:
        copy.wait()
    for side, target, is_last in ((0, to_other, jnp.logical_not(cols_are_even())), (1, to_partner, cols_are_even())):
        skip = jnp.where(is_last, 16, 0)
        packed = [jnp.zeros((8, LANES), I32)] * 2
        for k in range(12):
            moved = pltpu.roll(tiles[side, pl.ds(8 * k, 8), :], (16 * (k % 8) + skip) % LANES, 1)
            packed[k // 8] = jnp.where(lane // 16 == k % 8, moved, packed[k // 8])
        target[pl.ds(0, 8), :], target[pl.ds(8, 8), :] = packed


DEEP = 38
SIDE_AT = DEEP * GROUPS
MESSAGE = SIDE_AT + 16


def rows_kernel(lattice, draws, from_partner, from_other, side, near, far):
    lane = lax.broadcasted_iota(I32, (8, LANES), 1)
    partner_is_right = cols_are_even()
    low = (lane < LANES // 2) == partner_is_right
    for k in range(12):
        at = pl.ds(8 * (k // 8), 8)
        back = LANES - 16 * (k % 8)
        partner = pltpu.roll(from_partner[at, :], (back + jnp.where(partner_is_right, 0, LANES - 16)) % LANES, 1)
        other = pltpu.roll(from_other[at, :], (back + jnp.where(partner_is_right, LANES - 16, 0)) % LANES, 1)
        side[pl.ds(8 * k, 8), :] = jnp.where(low, partner, other)

    def write(target, down):
        below = (((2, 24), 30), ((1, 24), 23), ((1, 16), 15), ((0, 24), 8), ((0, 16), 0))
        above = (((0, 0), 0), ((0, 8), 8), ((1, 0), 16), ((1, 8), 24), ((2, 0), 31))
        for g in range(GROUPS):
            for (n, row), at in below if down else above:
                ref = lattice if n == 0 else draws.at[n - 1]
                target[pl.ds(DEEP * g + at, 8), :] = ref[pl.ds(row, 8), pl.ds(g * LANES, LANES)]
        start = 16 if down else 0
        dense = jnp.zeros((8, LANES), I32)
        for k, row in enumerate((start, start + 8, 32 + start, 40 + start, 88 if down else 64)):
            moved = pltpu.roll(side[pl.ds(row, 8), :], (32 * (k % 4) + 16) % LANES, 1)
            dense = jnp.where(lane // 32 == k % 4, moved, dense)
            if k >= 3:
                target[pl.ds(SIDE_AT + 8 * (k - 3), 8), :] = dense

    @pl.when(rows_are_even())
    def _():
        write(near, True)
        write(far, False)

    @pl.when(jnp.logical_not(rows_are_even()))
    def _():
        write(far, True)
        write(near, False)


def swap(x, axis, first, only=None):
    count = lax.axis_size(axis)
    pairs = [(i, (i + 1) % count) for i in range(first, count, 2)][only or slice(None)]
    return lax.ppermute(x, axis, pairs + [(j, i) for i, j in pairs])


def on_device(lattice, draws, thresholds):
    width = GROUPS * LANES
    vmem, smem = pl.BlockSpec(memory_space=pltpu.VMEM), pl.BlockSpec(memory_space=pltpu.SMEM)

    def call(kernel, out_shape, flops, args, **kwargs):
        return pl.pallas_call(
            kernel,
            out_shape=out_shape,
            compiler_params=pltpu.CompilerParams(vmem_limit_bytes=16 << 20),
            cost_estimate=pl.CostEstimate(flops=flops, bytes_accessed=2_000_000, transcendentals=0),
            **kwargs,
        )(*args)

    def words(*shape):
        return jax.ShapeDtypeStruct(shape, I32)

    to_partner, to_other = call(
        side_kernel,
        (words(16, LANES),) * 2,
        1_000_000,
        tuple(pltpu.with_memory_space_constraint(x, pltpu.HBM) for x in (lattice, draws)),
        in_specs=[pl.BlockSpec(memory_space=pltpu.HBM)] * 2,
        scratch_shapes=[pltpu.VMEM((2, 96, LANES), I32), pltpu.SemaphoreType.DMA((6,))],
    )
    from_other = swap(to_other, "cols", 1)
    from_partner = swap(to_partner, "cols", 0)

    side, to_near, to_far = call(
        rows_kernel,
        (words(96, LANES), words(MESSAGE, LANES), words(MESSAGE, LANES)),
        1_000_000,
        (lattice, draws, from_partner, from_other),
    )
    near_top = swap(to_near, "rows", 0, slice(0, 1))
    far = swap(to_far, "rows", 1)
    near = swap(to_near, "rows", 0, slice(1, None))

    accept, spins, table = call(
        own_kernel,
        (words(2, 2, SWEEPS, LEVELS, 8, LANES), words(2, 2, 8, LANES), words(2, 8, LEVELS, 8, LANES)),
        50_000_000,
        (thresholds, lattice, draws),
        in_specs=[smem, vmem, vmem],
        scratch_shapes=[pltpu.VMEM((32, 8, LANES), I32)],
    )

    final, means = call(
        sweep_kernel,
        (words(32, width), jax.ShapeDtypeStruct((1, 32), jnp.float32)),
        40_000_000,
        (near_top, near, far, side, spins, accept, table),
        in_specs=[vmem] * 7,
        out_specs=(pl.BlockSpec(memory_space=pltpu.HBM), vmem),
        scratch_shapes=[
            pltpu.VMEM((2, 2, 32, 8, LANES), I32),
            pltpu.VMEM((2, 32, 8, LANES), I32),
            pltpu.VMEM((32, 8, LANES), I32),
            pltpu.VMEM((3, 2, 8, LANES), I32),
            pltpu.VMEM((32, width), I32),
            pltpu.SemaphoreType.DMA((4,)),
        ],
    )
    return final, lax.psum(means, "cols").reshape(32)


def solution(mesh):
    in_specs = (P("rows", "cols"), P(None, "rows", "cols"), P())
    out_specs = (P("rows", "cols"), P("rows"))

    return jax.shard_map(on_device, mesh=mesh, in_specs=in_specs, out_specs=out_specs, check_vma=False)
```

```python
import jax
import jax.numpy as jnp
from jax import lax
from jax.experimental import pallas as pl
from jax.experimental.pallas import tpu as pltpu
from jax.sharding import PartitionSpec as P


SWEEPS = 8
LEVELS = 5
GROUPS = 32
LANES = 128
I32 = jnp.int32


def iotas():
    sub = lax.broadcasted_iota(I32, (8, LANES), 0)
    lane = lax.broadcasted_iota(I32, (8, LANES), 1)
    return sub, lane, (sub + lane) % 2 == 0


def srl(x, n):
    return lax.shift_right_logical(x, jnp.full(x.shape, n, I32))


def up_one(x):
    return pltpu.roll(x, 7, 0)


def split_colours(first, second, even):
    moved = up_one(second)
    return jnp.where(even, first, moved), jnp.where(even, moved, first)


def transpose_bits(words, low_half=False):
    a = list(words)
    masks = {16: 0x0000FFFF, 8: 0x00FF00FF, 4: 0x0F0F0F0F, 2: 0x33333333, 1: 0x55555555}
    for j in (16, 8, 4, 2, 1):
        m = jnp.int32(masks[j])
        for k in range(32):
            if k & j:
                continue
            if low_half and j == 16:
                a[k], a[k + j] = a[k] & m, srl(a[k], 16)
                continue
            t = (srl(a[k], j) ^ a[k + j]) & m
            a[k + j] = a[k + j] ^ t
            a[k] = a[k] ^ (t << j)
    return a


def pack_spins(load):
    word = srl(load(0), 1) & 1
    for g in range(1, GROUPS):
        bit = 1 << g if g < 31 else -(1 << 31)
        word = word | (load(g) & jnp.int32(bit))
    return word


def acceptance(u, table):
    r = []
    for k in range(LEVELS):
        z = table[0, 0, k]
        for b in range(8):
            z = (z & (u[b] ^ table[0, b, k])) ^ table[1, b, k]
        r.append(z)
    return r


def own_kernel(thresholds, lattice, draws, accept, words, table, planes):
    _, _, even = iotas()

    for k in range(LEVELS):
        clear = [((thresholds[LEVELS - 1 - k] - 1) >> b & 1) - 1 for b in range(8)]
        for b in range(8):
            table[0, b, k] = jnp.full((8, LANES), clear[b], I32)
            table[1, b, k] = jnp.full((8, LANES), clear[b] ^ (clear[b + 1] if b < 7 else -1), I32)

    def tile(ref, row, g):
        return ref[pl.ds(row, 8), pl.ds(g * LANES, LANES)]

    for q in range(2):
        first = pack_spins(lambda g: tile(lattice, 16 * q, g))
        second = pack_spins(lambda g: tile(lattice, 16 * q + 8, g))
        words[q, 0], words[q, 1] = split_colours(first, second, even)

    def body(n, carry):
        q, c, p = n // 4, n // 2 % 2, n % 2
        row = pl.multiple_of(q * 16, 16)
        mine = even == (c == 0)
        inputs = []
        for g in range(GROUPS):
            cols = pl.ds(g * LANES, LANES)
            inputs.append(jnp.where(mine, draws[p, pl.ds(row, 8), cols], up_one(draws[p, pl.ds(row + 8, 8), cols])))
        for b, plane in enumerate(transpose_bits(inputs)):
            planes[b] = plane

        def one_sweep(t, carry):
            u = [planes[8 * t + b] for b in range(8)]
            at = 4 * p + t
            for n, form in enumerate(acceptance(u, table)):
                accept[q, c, at, n] = form
            return carry

        return lax.fori_loop(0, 4, one_sweep, carry)

    lax.fori_loop(0, 8, body, 0)


def sweep_kernel(
    near_top, corner_top, near, far, side, words, accept, table, final, means, edge0, edge1, side_planes, packed, spins, sems
):
    sub, lane, even = iotas()
    odd = jnp.logical_not(even)

    def from_near(row):
        first = corner_top[pl.ds(row - SIDE_AT, 8), :] if row >= SIDE_AT else near_top[pl.ds(row, 8), :]
        return first | near[pl.ds(row, 8), :]

    def from_far(row):
        return far[pl.ds(row, 8), :]

    def read_edges(top, bot):
        for n, load in enumerate((top, bot)):
            first = pack_spins(lambda g: load(DEEP * g))
            second = pack_spins(lambda g: load(DEEP * g + 8))
            packed[n, 0], packed[n, 1] = split_colours(first, second, even)
            at = 15 if n == 0 else 16
            pairs = [split_colours(load(DEEP * g + at), load(DEEP * g + at + 8), even) for g in range(GROUPS)]
            for c in range(2):
                for b, plane in enumerate(transpose_bits([pair[c] for pair in pairs])):
                    edge0[n, c, b] = plane
        pairs = [split_colours(bot(DEEP * g + 31), top(DEEP * g + 30), even) for g in range(GROUPS)]
        for c in range(2):
            for b, plane in enumerate(transpose_bits([pair[c] for pair in pairs])):
                edge1[c, b] = plane

        outer = []
        for load in (top, bot):
            dense = (load(SIDE_AT), load(SIDE_AT + 8))
            outer.append([pltpu.roll(dense[k // 4], LANES - 16 - 32 * (k % 4), 1) for k in range(4)])
            outer[-1].append(pltpu.roll(dense[1], LANES - 16, 1))

        def side_tiles(q, n):
            if q in (0, 3):
                return outer[q // 3][2 * n], outer[q // 3][2 * n + 1]
            at = 32 * n + 16 * (q - 1)
            return side[pl.ds(at, 8), :], side[pl.ds(at + 8, 8), :]

        columns = [jnp.zeros((8, LANES), I32)] * 2
        slots = [jnp.zeros((8, LANES), I32)] * 32
        for q in range(4):
            pair = split_colours(*side_tiles(q, 0), even)
            for c in range(2):
                columns[c] = columns[c] | ((srl(pair[c], 1) & 1) << q)
            slots[q], slots[4 + q] = split_colours(*side_tiles(q, 1), even)
            second_word = (outer[1][4], outer[0][4]) if q in (0, 3) else side_tiles(q, 2)
            slots[8 + q], slots[12 + q] = split_colours(*second_word, even)
        packed[2, 0], packed[2, 1] = columns
        for b, plane in enumerate(transpose_bits(slots, low_half=True)):
            side_planes[b] = plane

    @pl.when(rows_are_even())
    def _():
        read_edges(from_far, from_near)

    @pl.when(jnp.logical_not(rows_are_even()))
    def _():
        read_edges(from_near, from_far)

    state = [[packed[0, c], words[0, c], words[1, c], packed[1, c], packed[2, c]] for c in range(2)]

    at_left, at_right = lane == 0, lane == LANES - 1
    fix = []
    for c in range(2):
        here, there = (even, odd) if c == 0 else (odd, even)
        fix.append((here & (sub == 0), there & (sub == 7), here & (sub == 7), there & (sub == 6)))

    def rules_of(c, t):
        p, at = t // 4, t % 4
        joined = p == 1
        blocks = (0, 1, 2, 4) if joined else (0, 1, 2, 3, 4)
        rules = {}
        for q in blocks:
            if q in (1, 2):
                rules[q] = [accept[q - 1, c, t, n] for n in range(LEVELS)]
                continue
            if q == 4:
                u = [srl(side_planes[8 * at + b], 8 * p + 4 * c) for b in range(8)]
            elif joined:
                u = [edge1[c, 8 * at + b] for b in range(8)]
            else:
                u = [edge0[q // 3, c, 8 * at + b] for b in range(8)]
            rules[q] = acceptance(u, table)
        return rules

    def half_sweep(mine, other, c, t, rules):
        p = t // 4
        joined = p == 1
        blocks = (0, 1, 2, 4) if joined else (0, 1, 2, 3, 4)
        up_prev, up_self, down_self, down_next = fix[c]
        left = {q: pltpu.roll(other[q], 1, 1) for q in blocks}
        right = {q: pltpu.roll(other[q], LANES - 1, 1) for q in blocks}
        side_left = jnp.zeros((8, LANES), I32)
        side_right = jnp.zeros((8, LANES), I32)
        for q in blocks[:-1]:
            if joined and q == 0:
                side_left = side_left | (srl(left[0], 31) * 9)
                side_right = side_right | ((right[0] & 1) * 9)
            else:
                side_left = side_left | (srl(left[q], 31) << q)
                side_right = side_right | ((right[q] & 1) << q)
        mine_first = even if c == 0 else odd
        new = {}
        for q in blocks:
            w, s = other[q], mine[q]
            if q < 4:
                if joined and q == 0:
                    from_left = jnp.where(mine_first, srl(left[4], 3), left[4]) & 1
                    from_right = jnp.where(mine_first, right[4] << 28, right[4] << 31) & jnp.int32(-(1 << 31))
                    before, after = other[2], other[1]
                else:
                    from_left = srl(left[4], q) & 1
                    from_right = (right[4] << (31 - q)) & jnp.int32(-(1 << 31))
                    before = other[max(q - 1, 0)]
                    after = other[0 if joined and q == 2 else min(q + 1, 3)]
                lft = jnp.where(at_left, (left[q] << 1) | from_left, left[q])
                rgt = jnp.where(at_right, srl(right[q], 1) | from_right, right[q])
                before, after = pltpu.roll(before, 2, 0), pltpu.roll(after, 6, 0)
            else:
                lft = jnp.where(at_left, side_left, left[4])
                rgt = jnp.where(at_right, side_right, right[4])
                before = pltpu.roll(w, 2, 0) << 1
                after = srl(pltpu.roll(w, 6, 0), 1)
            up = jnp.where(up_prev, before, jnp.where(up_self, w, pltpu.roll(w, 1, 0)))
            down = jnp.where(down_next, after, jnp.where(down_self, w, pltpu.roll(w, 7, 0)))
            lft, rgt, up, down = lft ^ s, rgt ^ s, up ^ s, down ^ s
            r = rules[q]
            one, two = up ^ down, up & down
            with_none = r[0] ^ (one & (r[0] ^ r[1])) ^ (two & (r[0] ^ r[2]))
            with_one = r[1] ^ (one & (r[1] ^ r[2])) ^ (two & (r[1] ^ r[3]))
            with_two = r[2] ^ (one & (r[2] ^ r[3])) ^ (two & (r[2] ^ r[4]))
            keep = s ^ with_none
            new[q] = keep ^ ((lft ^ rgt) & (with_none ^ with_one)) ^ ((lft & rgt) & (with_none ^ with_two))
        return new

    a, b = ({q: colour[q] for q in range(5)} for colour in state)
    rules = rules_of(0, 0)
    for t in range(SWEEPS):
        if t == 4:
            a[0] = jnp.where(even, a[3], a[0])
            b[0] = jnp.where(odd, b[3], b[0])
        after = rules_of(1, t)
        a = half_sweep(a, b, 0, t, rules)
        rules = rules_of(0, t + 1) if t < SWEEPS - 1 else None
        b = half_sweep(b, a, 1, t, after)

    copies = []
    tiles = []
    for q in (1, 2):
        first = jnp.where(even, a[q], b[q])
        second = pltpu.roll(jnp.where(even, b[q], a[q]), 1, 0)
        for n, word in enumerate((first, second)):
            row = 16 * (q - 1) + 8 * n
            for g in range(GROUPS):
                spins[pl.ds(row, 8), pl.ds(g * LANES, LANES)] = ((word << (31 - g)) >> 31) | 1
            at = pl.ds(row, 8)
            copies.append(pltpu.make_async_copy(spins.at[at], final.at[at], sems.at[len(copies)]))
            copies[-1].start()
            tiles.append((row, word))
    sums = jnp.zeros((8, LANES), jnp.float32)
    for row, word in tiles:
        minus = jnp.sum(lax.population_count(word).astype(jnp.float32), axis=1, keepdims=True)
        mean = (GROUPS * LANES - 2.0 * minus) * (1.0 / (4 * GROUPS * LANES))
        sums = sums + jnp.where(lane == row + sub, mean, 0.0)
    means[...] = jnp.sum(sums, axis=0, keepdims=True)[:, :32]
    for copy in copies:
        copy.wait()


def rows_are_even():
    return lax.axis_index("rows") % 2 == 0


def cols_are_even():
    return lax.axis_index("cols") % 2 == 0


def side_kernel(lattice, draws, to_partner, to_other, tiles, sem):
    lane = lax.broadcasted_iota(I32, (8, LANES), 1)
    last = (GROUPS - 1) * LANES
    copies = []
    for side, is_last in enumerate((jnp.logical_not(cols_are_even()), cols_are_even())):
        column = pl.ds(pl.multiple_of(jnp.where(is_last, last, 0), LANES), LANES)
        for n, ref in enumerate((lattice, draws.at[0], draws.at[1])):
            target = tiles.at[side, pl.ds(32 * n, 32), :]
            copies.append(pltpu.make_async_copy(ref.at[:, column], target, sem.at[len(copies)]))
            copies[-1].start()
    for side, target, is_last in ((0, to_other, jnp.logical_not(cols_are_even())), (1, to_partner, cols_are_even())):
        for copy in copies[3 * side : 3 * side + 3]:
            copy.wait()
        skip = jnp.where(is_last, 16, 0)
        packed = [jnp.zeros((8, LANES), I32)] * 2
        for k in range(12):
            moved = pltpu.roll(tiles[side, pl.ds(8 * k, 8), :], (16 * (k % 8) + skip) % LANES, 1)
            packed[k // 8] = jnp.where(lane // 16 == k % 8, moved, packed[k // 8])
        target[pl.ds(0, 8), :], target[pl.ds(8, 8), :] = packed


DEEP = 38
SIDE_AT = DEEP * GROUPS
MESSAGE = SIDE_AT + 16


def write_rows(lattice, draws, target, down):
    below = (((2, 24), 30), ((1, 24), 23), ((1, 16), 15), ((0, 24), 8), ((0, 16), 0))
    above = (((0, 0), 0), ((0, 8), 8), ((1, 0), 16), ((1, 8), 24), ((2, 0), 31))
    for g in range(GROUPS):
        for (n, row), at in below if down else above:
            ref = lattice if n == 0 else draws.at[n - 1]
            target[pl.ds(DEEP * g + at, 8), :] = ref[pl.ds(row, 8), pl.ds(g * LANES, LANES)]


def top_kernel(lattice, draws, top):
    @pl.when(rows_are_even())
    def _():
        write_rows(lattice, draws, top, True)

    @pl.when(jnp.logical_not(rows_are_even()))
    def _():
        write_rows(lattice, draws, top, False)


def rows_kernel(lattice, draws, from_partner, from_other, side, near, far, corner):
    lane = lax.broadcasted_iota(I32, (8, LANES), 1)
    partner_is_right = cols_are_even()
    low = (lane < LANES // 2) == partner_is_right
    for k in range(12):
        at = pl.ds(8 * (k // 8), 8)
        back = LANES - 16 * (k % 8)
        partner = pltpu.roll(from_partner[at, :], (back + jnp.where(partner_is_right, 0, LANES - 16)) % LANES, 1)
        other = pltpu.roll(from_other[at, :], (back + jnp.where(partner_is_right, LANES - 16, 0)) % LANES, 1)
        side[pl.ds(8 * k, 8), :] = jnp.where(low, partner, other)

    def write(target, down):
        write_rows(lattice, draws, target, down)
        start = 16 if down else 0
        dense = jnp.zeros((8, LANES), I32)
        for k, row in enumerate((start, start + 8, 32 + start, 40 + start, 88 if down else 64)):
            moved = pltpu.roll(side[pl.ds(row, 8), :], (32 * (k % 4) + 16) % LANES, 1)
            dense = jnp.where(lane // 32 == k % 4, moved, dense)
            if k >= 3:
                target[pl.ds(SIDE_AT + 8 * (k - 3), 8), :] = dense

    @pl.when(rows_are_even())
    def _():
        write(near, True)
        write(far, False)

    @pl.when(jnp.logical_not(rows_are_even()))
    def _():
        write(far, True)
        write(near, False)

    corner[...] = near[pl.ds(SIDE_AT, 16), :]


def swap(x, axis, first, only=None):
    count = lax.axis_size(axis)
    pairs = [(i, (i + 1) % count) for i in range(first, count, 2)][only or slice(None)]
    return lax.ppermute(x, axis, pairs + [(j, i) for i, j in pairs])


def on_device(lattice, draws, thresholds):
    width = GROUPS * LANES
    vmem, smem = pl.BlockSpec(memory_space=pltpu.VMEM), pl.BlockSpec(memory_space=pltpu.SMEM)

    def call(kernel, out_shape, flops, args, **kwargs):
        return pl.pallas_call(
            kernel,
            out_shape=out_shape,
            compiler_params=pltpu.CompilerParams(vmem_limit_bytes=16 << 20),
            cost_estimate=pl.CostEstimate(flops=flops, bytes_accessed=2_000_000, transcendentals=0),
            **kwargs,
        )(*args)

    def words(*shape):
        return jax.ShapeDtypeStruct(shape, I32)

    to_partner, to_other = call(
        side_kernel,
        (words(16, LANES),) * 2,
        1_000_000,
        tuple(pltpu.with_memory_space_constraint(x, pltpu.HBM) for x in (lattice, draws)),
        in_specs=[pl.BlockSpec(memory_space=pltpu.HBM)] * 2,
        scratch_shapes=[pltpu.VMEM((2, 96, LANES), I32), pltpu.SemaphoreType.DMA((6,))],
    )
    from_other = swap(to_other, "cols", 1)
    from_partner = swap(to_partner, "cols", 0)

    to_top = call(top_kernel, words(SIDE_AT + 8, LANES), 1_000_000, (lattice, draws))
    near_top = swap(to_top, "rows", 0, slice(0, 1))
    side, to_near, to_far, to_corner = call(
        rows_kernel,
        (words(96, LANES), words(MESSAGE, LANES), words(MESSAGE, LANES), words(16, LANES)),
        1_000_000,
        (lattice, draws, from_partner, from_other),
    )
    far = swap(to_far, "rows", 1)
    near = swap(to_near, "rows", 0, slice(1, None))

    corner_top = swap(to_corner, "rows", 0, slice(0, 1))

    accept, spins, table = call(
        own_kernel,
        (words(2, 2, SWEEPS, LEVELS, 8, LANES), words(2, 2, 8, LANES), words(2, 8, LEVELS, 8, LANES)),
        50_000_000,
        (thresholds, lattice, draws),
        in_specs=[smem, vmem, vmem],
        scratch_shapes=[pltpu.VMEM((32, 8, LANES), I32)],
    )

    final, means = call(
        sweep_kernel,
        (words(32, width), jax.ShapeDtypeStruct((1, 32), jnp.float32)),
        40_000_000,
        (near_top, corner_top, near, far, side, spins, accept, table),
        in_specs=[vmem] * 8,
        out_specs=(pl.BlockSpec(memory_space=pltpu.HBM), vmem),
        scratch_shapes=[
            pltpu.VMEM((2, 2, 32, 8, LANES), I32),
            pltpu.VMEM((2, 32, 8, LANES), I32),
            pltpu.VMEM((32, 8, LANES), I32),
            pltpu.VMEM((3, 2, 8, LANES), I32),
            pltpu.VMEM((32, width), I32),
            pltpu.SemaphoreType.DMA((4,)),
        ],
    )
    return final, lax.psum(means, "cols").reshape(32)


def solution(mesh):
    in_specs = (P("rows", "cols"), P(None, "rows", "cols"), P())
    out_specs = (P("rows", "cols"), P("rows"))

    return jax.shard_map(on_device, mesh=mesh, in_specs=in_specs, out_specs=out_specs, check_vma=False)
```

```python
import jax
import jax.numpy as jnp
from jax import lax
from jax.experimental import pallas as pl
from jax.experimental.pallas import tpu as pltpu
from jax.sharding import PartitionSpec as P


SWEEPS = 8
LEVELS = 5
GROUPS = 32
LANES = 128
I32 = jnp.int32


def iotas():
    sub = lax.broadcasted_iota(I32, (8, LANES), 0)
    lane = lax.broadcasted_iota(I32, (8, LANES), 1)
    return sub, lane, (sub + lane) % 2 == 0


def srl(x, n):
    return lax.shift_right_logical(x, jnp.full(x.shape, n, I32))


def up_one(x):
    return pltpu.roll(x, 7, 0)


def split_colours(first, second, even):
    moved = up_one(second)
    return jnp.where(even, first, moved), jnp.where(even, moved, first)


def transpose_bits(words, low_half=False):
    a = list(words)
    masks = {16: 0x0000FFFF, 8: 0x00FF00FF, 4: 0x0F0F0F0F, 2: 0x33333333, 1: 0x55555555}
    for j in (16, 8, 4, 2, 1):
        m = jnp.int32(masks[j])
        for k in range(32):
            if k & j:
                continue
            if low_half and j == 16:
                a[k], a[k + j] = a[k] & m, srl(a[k], 16)
                continue
            t = (srl(a[k], j) ^ a[k + j]) & m
            a[k + j] = a[k + j] ^ t
            a[k] = a[k] ^ (t << j)
    return a


def pack_spins(load):
    word = srl(load(0), 1) & 1
    for g in range(1, GROUPS):
        bit = 1 << g if g < 31 else -(1 << 31)
        word = word | (load(g) & jnp.int32(bit))
    return word


def acceptance(u, table):
    r = []
    for k in range(LEVELS):
        z = table[0, 0, k]
        for b in range(8):
            z = (z & (u[b] ^ table[0, b, k])) ^ table[1, b, k]
        r.append(z)
    return r


def own_kernel(thresholds, lattice, draws, accept, words, table, planes):
    _, _, even = iotas()

    for k in range(LEVELS):
        clear = [((thresholds[LEVELS - 1 - k] - 1) >> b & 1) - 1 for b in range(8)]
        for b in range(8):
            table[0, b, k] = jnp.full((8, LANES), clear[b], I32)
            table[1, b, k] = jnp.full((8, LANES), clear[b] ^ (clear[b + 1] if b < 7 else -1), I32)

    def tile(ref, row, g):
        return ref[pl.ds(row, 8), pl.ds(g * LANES, LANES)]

    for q in range(2):
        first = pack_spins(lambda g: tile(lattice, 16 * q, g))
        second = pack_spins(lambda g: tile(lattice, 16 * q + 8, g))
        words[q, 0], words[q, 1] = split_colours(first, second, even)

    def body(n, carry):
        q, c, p = n // 4, n // 2 % 2, n % 2
        row = pl.multiple_of(q * 16, 16)
        mine = even == (c == 0)
        inputs = []
        for g in range(GROUPS):
            cols = pl.ds(g * LANES, LANES)
            inputs.append(jnp.where(mine, draws[p, pl.ds(row, 8), cols], up_one(draws[p, pl.ds(row + 8, 8), cols])))
        for b, plane in enumerate(transpose_bits(inputs)):
            planes[b] = plane

        def one_sweep(t, carry):
            u = [planes[8 * t + b] for b in range(8)]
            at = 4 * p + t
            for n, form in enumerate(acceptance(u, table)):
                accept[q, c, at, n] = form
            return carry

        return lax.fori_loop(0, 4, one_sweep, carry)

    lax.fori_loop(0, 8, body, 0)


def sweep_kernel(
    near_top, corner_top, near, far, side, words, accept, table, final, means, edge0, edge1, side_planes, packed, spins, sems
):
    sub, lane, even = iotas()
    odd = jnp.logical_not(even)

    def from_near(row):
        first = corner_top[pl.ds(row - SIDE_AT, 8), :] if row >= SIDE_AT else near_top[pl.ds(row, 8), :]
        return first | near[pl.ds(row, 8), :]

    def from_far(row):
        return far[pl.ds(row, 8), :]

    def read_edges(top, bot):
        for n, load in enumerate((top, bot)):
            first = pack_spins(lambda g: load(DEEP * g))
            second = pack_spins(lambda g: load(DEEP * g + 8))
            packed[n, 0], packed[n, 1] = split_colours(first, second, even)
            at = 15 if n == 0 else 16
            pairs = [split_colours(load(DEEP * g + at), load(DEEP * g + at + 8), even) for g in range(GROUPS)]
            for c in range(2):
                for b, plane in enumerate(transpose_bits([pair[c] for pair in pairs])):
                    edge0[n, c, b] = plane
        pairs = [split_colours(bot(DEEP * g + 31), top(DEEP * g + 30), even) for g in range(GROUPS)]
        for c in range(2):
            for b, plane in enumerate(transpose_bits([pair[c] for pair in pairs])):
                edge1[c, b] = plane

        outer = []
        for load in (top, bot):
            dense = (load(SIDE_AT), load(SIDE_AT + 8))
            outer.append([pltpu.roll(dense[k // 4], LANES - 16 - 32 * (k % 4), 1) for k in range(4)])
            outer[-1].append(pltpu.roll(dense[1], LANES - 16, 1))

        def side_tiles(q, n):
            if q in (0, 3):
                return outer[q // 3][2 * n], outer[q // 3][2 * n + 1]
            at = 32 * n + 16 * (q - 1)
            return side[pl.ds(at, 8), :], side[pl.ds(at + 8, 8), :]

        columns = [jnp.zeros((8, LANES), I32)] * 2
        slots = [jnp.zeros((8, LANES), I32)] * 32
        for q in range(4):
            pair = split_colours(*side_tiles(q, 0), even)
            for c in range(2):
                columns[c] = columns[c] | ((srl(pair[c], 1) & 1) << q)
            slots[q], slots[4 + q] = split_colours(*side_tiles(q, 1), even)
            second_word = (outer[1][4], outer[0][4]) if q in (0, 3) else side_tiles(q, 2)
            slots[8 + q], slots[12 + q] = split_colours(*second_word, even)
        packed[2, 0], packed[2, 1] = columns
        for b, plane in enumerate(transpose_bits(slots, low_half=True)):
            side_planes[b] = plane

    @pl.when(rows_are_even())
    def _():
        read_edges(from_far, from_near)

    @pl.when(jnp.logical_not(rows_are_even()))
    def _():
        read_edges(from_near, from_far)

    state = [[packed[0, c], words[0, c], words[1, c], packed[1, c], packed[2, c]] for c in range(2)]

    at_left, at_right = lane == 0, lane == LANES - 1
    fix = []
    for c in range(2):
        here, there = (even, odd) if c == 0 else (odd, even)
        fix.append((here & (sub == 0), there & (sub == 7), here & (sub == 7), there & (sub == 6)))

    def rules_of(c, t):
        p, at = t // 4, t % 4
        joined = p == 1
        blocks = (0, 1, 2, 4) if joined else (0, 1, 2, 3, 4)
        rules = {}
        for q in blocks:
            if q in (1, 2):
                rules[q] = [accept[q - 1, c, t, n] for n in range(LEVELS)]
                continue
            if q == 4:
                u = [srl(side_planes[8 * at + b], 8 * p + 4 * c) for b in range(8)]
            elif joined:
                u = [edge1[c, 8 * at + b] for b in range(8)]
            else:
                u = [edge0[q // 3, c, 8 * at + b] for b in range(8)]
            rules[q] = acceptance(u, table)
        return rules

    def half_sweep(mine, other, c, t, rules):
        p = t // 4
        joined = p == 1
        blocks = (0, 1, 2, 4) if joined else (0, 1, 2, 3, 4)
        up_prev, up_self, down_self, down_next = fix[c]
        left = {q: pltpu.roll(other[q], 1, 1) for q in blocks}
        right = {q: pltpu.roll(other[q], LANES - 1, 1) for q in blocks}
        side_left = jnp.zeros((8, LANES), I32)
        side_right = jnp.zeros((8, LANES), I32)
        for q in blocks[:-1]:
            if joined and q == 0:
                side_left = side_left | (srl(left[0], 31) * 9)
                side_right = side_right | ((right[0] & 1) * 9)
            else:
                side_left = side_left | (srl(left[q], 31) << q)
                side_right = side_right | ((right[q] & 1) << q)
        mine_first = even if c == 0 else odd
        new = {}
        for q in blocks:
            w, s = other[q], mine[q]
            if q < 4:
                if joined and q == 0:
                    from_left = jnp.where(mine_first, srl(left[4], 3), left[4]) & 1
                    from_right = jnp.where(mine_first, right[4] << 28, right[4] << 31) & jnp.int32(-(1 << 31))
                    before, after = other[2], other[1]
                else:
                    from_left = srl(left[4], q) & 1
                    from_right = (right[4] << (31 - q)) & jnp.int32(-(1 << 31))
                    before = other[max(q - 1, 0)]
                    after = other[0 if joined and q == 2 else min(q + 1, 3)]
                lft = jnp.where(at_left, (left[q] << 1) | from_left, left[q])
                rgt = jnp.where(at_right, srl(right[q], 1) | from_right, right[q])
                before, after = pltpu.roll(before, 2, 0), pltpu.roll(after, 6, 0)
            else:
                lft = jnp.where(at_left, side_left, left[4])
                rgt = jnp.where(at_right, side_right, right[4])
                before = pltpu.roll(w, 2, 0) << 1
                after = srl(pltpu.roll(w, 6, 0), 1)
            up = jnp.where(up_prev, before, jnp.where(up_self, w, pltpu.roll(w, 1, 0)))
            down = jnp.where(down_next, after, jnp.where(down_self, w, pltpu.roll(w, 7, 0)))
            lft, rgt, up, down = lft ^ s, rgt ^ s, up ^ s, down ^ s
            r = rules[q]
            one, two = up ^ down, up & down
            with_none = r[0] ^ (one & (r[0] ^ r[1])) ^ (two & (r[0] ^ r[2]))
            with_one = r[1] ^ (one & (r[1] ^ r[2])) ^ (two & (r[1] ^ r[3]))
            with_two = r[2] ^ (one & (r[2] ^ r[3])) ^ (two & (r[2] ^ r[4]))
            keep = s ^ with_none
            new[q] = keep ^ ((lft ^ rgt) & (with_none ^ with_one)) ^ ((lft & rgt) & (with_none ^ with_two))
        return new

    a, b = ({q: colour[q] for q in range(5)} for colour in state)
    rules = rules_of(0, 0)
    for t in range(SWEEPS):
        if t == 4:
            a[0] = jnp.where(even, a[3], a[0])
            b[0] = jnp.where(odd, b[3], b[0])
        after = rules_of(1, t)
        a = half_sweep(a, b, 0, t, rules)
        rules = rules_of(0, t + 1) if t < SWEEPS - 1 else None
        b = half_sweep(b, a, 1, t, after)

    copies = []
    tiles = []
    for q in (1, 2):
        first = jnp.where(even, a[q], b[q])
        second = pltpu.roll(jnp.where(even, b[q], a[q]), 1, 0)
        for n, word in enumerate((first, second)):
            row = 16 * (q - 1) + 8 * n
            for g in range(GROUPS):
                spins[pl.ds(row, 8), pl.ds(g * LANES, LANES)] = ((word << (31 - g)) >> 31) | 1
            at = pl.ds(row, 8)
            copies.append(pltpu.make_async_copy(spins.at[at], final.at[at], sems.at[len(copies)]))
            copies[-1].start()
            tiles.append((row, word))
    sums = jnp.zeros((8, LANES), jnp.float32)
    for row, word in tiles:
        minus = jnp.sum(lax.population_count(word).astype(jnp.float32), axis=1, keepdims=True)
        mean = (GROUPS * LANES - 2.0 * minus) * (1.0 / (4 * GROUPS * LANES))
        sums = sums + jnp.where(lane == row + sub, mean, 0.0)
    means[...] = jnp.sum(sums, axis=0, keepdims=True)[:, :32]
    for copy in copies:
        copy.wait()


def rows_are_even():
    return lax.axis_index("rows") % 2 == 0


def cols_are_even():
    return lax.axis_index("cols") % 2 == 0


def side_kernel(lattice, draws, to_partner, to_other, tiles, sem):
    lane = lax.broadcasted_iota(I32, (8, LANES), 1)
    last = (GROUPS - 1) * LANES
    copies = []
    for side, is_last in enumerate((jnp.logical_not(cols_are_even()), cols_are_even())):
        column = pl.ds(pl.multiple_of(jnp.where(is_last, last, 0), LANES), LANES)
        for n, ref in enumerate((lattice, draws.at[0], draws.at[1])):
            target = tiles.at[side, pl.ds(32 * n, 32), :]
            copies.append(pltpu.make_async_copy(ref.at[:, column], target, sem.at[len(copies)]))
            copies[-1].start()
    for side, target, is_last in ((0, to_other, jnp.logical_not(cols_are_even())), (1, to_partner, cols_are_even())):
        for copy in copies[3 * side : 3 * side + 3]:
            copy.wait()
        skip = jnp.where(is_last, 16, 0)
        packed = [jnp.zeros((8, LANES), I32)] * 2
        for k in range(12):
            moved = pltpu.roll(tiles[side, pl.ds(8 * k, 8), :], (16 * (k % 8) + skip) % LANES, 1)
            packed[k // 8] = jnp.where(lane // 16 == k % 8, moved, packed[k // 8])
        target[pl.ds(0, 8), :], target[pl.ds(8, 8), :] = packed


DEEP = 38
SIDE_AT = DEEP * GROUPS
MESSAGE = SIDE_AT + 16


def write_rows(lattice, draws, target, down):
    below = (((2, 24), 30), ((1, 24), 23), ((1, 16), 15), ((0, 24), 8), ((0, 16), 0))
    above = (((0, 0), 0), ((0, 8), 8), ((1, 0), 16), ((1, 8), 24), ((2, 0), 31))
    for g in range(GROUPS):
        for (n, row), at in below if down else above:
            ref = lattice if n == 0 else draws.at[n - 1]
            target[pl.ds(DEEP * g + at, 8), :] = ref[pl.ds(row, 8), pl.ds(g * LANES, LANES)]


def main_kernel(lattice, draws, top, near, far):
    @pl.when(rows_are_even())
    def _():
        write_rows(lattice, draws, top, True)
        write_rows(lattice, draws, near, True)
        write_rows(lattice, draws, far, False)

    @pl.when(jnp.logical_not(rows_are_even()))
    def _():
        write_rows(lattice, draws, top, False)
        write_rows(lattice, draws, near, False)
        write_rows(lattice, draws, far, True)


def rows_kernel(from_partner, from_other, near_main, far_main, side, near, far, corner):
    lane = lax.broadcasted_iota(I32, (8, LANES), 1)
    partner_is_right = cols_are_even()
    low = (lane < LANES // 2) == partner_is_right
    for k in range(12):
        at = pl.ds(8 * (k // 8), 8)
        back = LANES - 16 * (k % 8)
        partner = pltpu.roll(from_partner[at, :], (back + jnp.where(partner_is_right, 0, LANES - 16)) % LANES, 1)
        other = pltpu.roll(from_other[at, :], (back + jnp.where(partner_is_right, LANES - 16, 0)) % LANES, 1)
        side[pl.ds(8 * k, 8), :] = jnp.where(low, partner, other)

    def write(target, down):
        start = 16 if down else 0
        dense = jnp.zeros((8, LANES), I32)
        for k, row in enumerate((start, start + 8, 32 + start, 40 + start, 88 if down else 64)):
            moved = pltpu.roll(side[pl.ds(row, 8), :], (32 * (k % 4) + 16) % LANES, 1)
            dense = jnp.where(lane // 32 == k % 4, moved, dense)
            if k >= 3:
                target[pl.ds(SIDE_AT + 8 * (k - 3), 8), :] = dense

    @pl.when(rows_are_even())
    def _():
        write(near, True)
        write(far, False)

    @pl.when(jnp.logical_not(rows_are_even()))
    def _():
        write(far, True)
        write(near, False)

    corner[...] = near[pl.ds(SIDE_AT, 16), :]


def swap(x, axis, first, only=None):
    count = lax.axis_size(axis)
    pairs = [(i, (i + 1) % count) for i in range(first, count, 2)][only or slice(None)]
    return lax.ppermute(x, axis, pairs + [(j, i) for i, j in pairs])


def on_device(lattice, draws, thresholds):
    width = GROUPS * LANES
    vmem, smem = pl.BlockSpec(memory_space=pltpu.VMEM), pl.BlockSpec(memory_space=pltpu.SMEM)

    def call(kernel, out_shape, flops, args, **kwargs):
        return pl.pallas_call(
            kernel,
            out_shape=out_shape,
            compiler_params=pltpu.CompilerParams(vmem_limit_bytes=16 << 20),
            cost_estimate=pl.CostEstimate(flops=flops, bytes_accessed=2_000_000, transcendentals=0),
            **kwargs,
        )(*args)

    def words(*shape):
        return jax.ShapeDtypeStruct(shape, I32)

    to_partner, to_other = call(
        side_kernel,
        (words(16, LANES),) * 2,
        1_000_000,
        tuple(pltpu.with_memory_space_constraint(x, pltpu.HBM) for x in (lattice, draws)),
        in_specs=[pl.BlockSpec(memory_space=pltpu.HBM)] * 2,
        scratch_shapes=[pltpu.VMEM((2, 96, LANES), I32), pltpu.SemaphoreType.DMA((6,))],
    )
    from_other = swap(to_other, "cols", 1)
    from_partner = swap(to_partner, "cols", 0)

    message = words(MESSAGE, LANES)
    to_top, near_main, far_main = call(main_kernel, (words(SIDE_AT + 8, LANES), message, message), 1_000_000, (lattice, draws))
    near_top = swap(to_top, "rows", 0, slice(0, 1))
    side, to_near, to_far, to_corner = call(
        rows_kernel,
        (words(96, LANES), message, message, words(16, LANES)),
        1_000_000,
        (from_partner, from_other, near_main, far_main),
        input_output_aliases={2: 1, 3: 2},
    )
    far = swap(to_far, "rows", 1)
    near = swap(to_near, "rows", 0, slice(1, None))

    corner_top = swap(to_corner, "rows", 0, slice(0, 1))

    accept, spins, table = call(
        own_kernel,
        (words(2, 2, SWEEPS, LEVELS, 8, LANES), words(2, 2, 8, LANES), words(2, 8, LEVELS, 8, LANES)),
        50_000_000,
        (thresholds, lattice, draws),
        in_specs=[smem, vmem, vmem],
        scratch_shapes=[pltpu.VMEM((32, 8, LANES), I32)],
    )

    final, means = call(
        sweep_kernel,
        (words(32, width), jax.ShapeDtypeStruct((1, 32), jnp.float32)),
        40_000_000,
        (near_top, corner_top, near, far, side, spins, accept, table),
        in_specs=[vmem] * 8,
        out_specs=(pl.BlockSpec(memory_space=pltpu.HBM), vmem),
        scratch_shapes=[
            pltpu.VMEM((2, 2, 32, 8, LANES), I32),
            pltpu.VMEM((2, 32, 8, LANES), I32),
            pltpu.VMEM((32, 8, LANES), I32),
            pltpu.VMEM((3, 2, 8, LANES), I32),
            pltpu.VMEM((32, width), I32),
            pltpu.SemaphoreType.DMA((4,)),
        ],
    )
    return final, lax.psum(means, "cols").reshape(32)


def solution(mesh):
    in_specs = (P("rows", "cols"), P(None, "rows", "cols"), P())
    out_specs = (P("rows", "cols"), P("rows"))

    return jax.shard_map(on_device, mesh=mesh, in_specs=in_specs, out_specs=out_specs, check_vma=False)
```
